32 devices in a mesh: groups: 2 (over x), freq: 16 (over z, y, core).
Axes of the slice: x: 2, y: 2, z: 4, core: 2. Of those that a mesh axis runs over, the one named last changes fastest.
Arguments:
- traces: bfloat16 [1024, 2048, 32], P('freq', None, 'groups'), parts along dimension 2, may hold values from -6 to 6
- freq_index: int32 [16], replicated, may hold values from 1 to 511
- block_map: int32 [64, 64], replicated, may hold values 0 or 1
- green_rec: bfloat16 [16, 2, 2048, 1536], P('freq', None, None, 'groups'), parts along dimension 3, may hold values from -0.1875 to 0.1875
- green_src: bfloat16 [16, 2, 16, 1536], P('freq', None, None, 'groups'), parts along dimension 3, may hold values from -0.25 to 0.25
Outputs:
- image: float32 [1536], P(('groups', 'freq')), parts along dimension 0
The draws below stay inside these ranges and needn't reach their ends.
There are 2 independent parts, one for each index of `groups`. The reference program is written for one: setup_inputs(seed, part) draws one part's arguments, and reference() takes and returns one part's arrays. A program takes and returns all parts, laid end to end along the dimension named above; an argument that names none is the same for every part. Nothing has to cross between parts.
Inputs may be any that keep to these rules, and one draw needn't show every extreme that they name: `freq_index`: frequency bins; they may repeat. `block_map`: 1 where a receiver block lies in an image tile's aperture.
All inputs are finite; a program needn't handle non-finite values.
Results may differ from the reference program's by a relative error of at most 0.0038.
Values may be sent and summed in bfloat16 or wider, within the bound.
A program may use at most 64 MiB of HBM per device.

```python
import math
import jax
import jax.numpy as jnp
from jax import lax

NT = 1024
R = 2048
RBLK = 64
TILES = 64
P_SIZE = 768
S = 16
FREQS = 16


def place_ends(result, key, low, largest):
    extent = result.shape
    spot = [jax.random.randint(jax.random.fold_in(key, axis), (), 0, extent[axis]) for axis in range(len(extent))]
    result = result.at[tuple(spot)].set(low)
    longest = extent.index(max(extent))
    spot[longest] = (spot[longest] + 1) % extent[longest]
    return result.at[tuple(spot)].set(largest)


def strengthened(entries, stream_key, source, target, shards_of, factor):
    owner, partner = [(jnp.arange(entries.shape[axis_at]) // (entries.shape[axis_at] // shards_of)).reshape([-1 if axis == axis_at else 1 for axis in range(entries.ndim)]) for axis_at in (source, target)]
    chosen = jax.random.permutation(stream_key, shards_of)[partner]
    strong = (owner == chosen) | (owner == (partner + shards_of // 2) % shards_of)
    return jnp.where(strong, factor * entries, entries)


def block_levels(key, shape, split, smallest, top_value):
    def one(position, blocks):
        heights = jax.random.uniform(jax.random.fold_in(jax.random.fold_in(key, 6), position), (blocks,), jnp.float32, smallest / len(split), top_value / len(split))
        return jnp.repeat(jnp.exp(heights), shape[position] // blocks).reshape((-1,) + (1,) * (len(shape) - position - 1))

    gain = one(*split[0])
    for cut in split[1:]:
        gain = gain * one(*cut)
    return gain


def centred(key, dims, width, bound, pieces=(), held_as=jnp.bfloat16):
    array = jax.random.normal(key, dims, jnp.float32) * width
    if len(pieces) > 0:
        array = block_levels(key, dims, pieces, -0.22, 0.18) * array
    return jnp.clip(array, min=-bound, max=bound).astype(held_as)


def gaussian_with(rng, extent, width, most, shards, heavy, kind=jnp.bfloat16):
    entries = width * jax.random.normal(rng, extent, jnp.float32)
    if shards:
        entries = entries * block_levels(rng, extent, shards, -0.22, 0.18)
    return jnp.clip(strengthened(entries, jax.random.fold_in(rng, 3), *heavy), -most, most).astype(kind)


def setup_inputs(seed: int = 0, part: int = 0) -> dict:
    key_of = jax.random.split(jax.random.key(seed), 6)
    part_keys = jax.random.split(jax.random.fold_in(key_of[5], part), 6)
    return {
        "traces": gaussian_with(part_keys[0], (NT, R, S), 1.0, 6.0, ((0, 16),), (0, 1, 16, 2.0)),
        "freq_index": place_ends(jax.random.randint(key_of[1], (FREQS,), 1, NT // 2), jax.random.fold_in(key_of[1], 1), 1, (NT // 2) - 1).astype(jnp.int32),
        "block_map": place_ends((jax.random.randint(key_of[2], (RBLK, TILES), 0, 3) < 1).astype(jnp.int32), jax.random.fold_in(key_of[2], 1), 0, 1),
        "green_rec": gaussian_with(part_keys[3], (FREQS, 2, R, P_SIZE), R ** -0.5, 0.1875, ((0, 16),), (0, 3, 16, 2.0)),
        "green_src": centred(part_keys[4], (FREQS, 2, S, P_SIZE), (2 * S * FREQS) ** -0.5, 0.25, ((0, 16),)),
    }


def dft_table(freq_index, length):
    sample_index = jnp.arange(length, dtype=jnp.int32)
    phases = freq_index[:, None] * sample_index[None, :] % length
    angles = phases.astype(jnp.float32) * jnp.float32(2.0 * math.pi / length)
    stacked = jnp.stack((jnp.cos(angles), -jnp.sin(angles)), axis=1)
    return stacked.reshape(freq_index.shape[0] * 2, length).astype(jnp.bfloat16)

def expand_map(block_map, receivers, points):
    row_span = receivers // block_map.shape[0]
    col_span = points // block_map.shape[1]
    return jnp.repeat(jnp.repeat(block_map, row_span, axis=0), col_span, axis=1).astype(jnp.bfloat16)

def reference(traces, freq_index, block_map, green_rec, green_src):
    cos_table = dft_table(freq_index, NT)
    spectrum = jnp.dot(cos_table, traces.reshape(NT, R * S), preferred_element_type=jnp.float32)
    spectrum = (spectrum * (1.0 / math.sqrt(NT))).astype(jnp.bfloat16).reshape(FREQS, 2, R, S)
    mask_full = expand_map(block_map, R, P_SIZE)

    def per_freq(image_sum, stacked):
        spec_f, rec_f, src_f = stacked
        masked = (rec_f * mask_full[None]).astype(jnp.float32)
        spec_w = spec_f.astype(jnp.float32)
        swapped = jnp.stack((spec_w[1], -spec_w[0]), axis=0)
        blocks = jnp.stack((spec_w, swapped), axis=0)
        back_field = jnp.einsum('crx,ocrs->osx', masked, blocks, precision=lax.Precision.HIGHEST)
        image_sum = image_sum + lax.optimization_barrier(jnp.sum(src_f.astype(jnp.float32) * back_field, axis=(0, 1)))
        return (image_sum, None)
    image, _ = lax.scan(per_freq, jnp.zeros((P_SIZE,), jnp.float32), (spectrum, green_rec, green_src))
    return image
```

```python
import math

import jax
import jax.numpy as jnp
from jax import lax
from jax.experimental import pallas as pl
from jax.experimental.pallas import tpu as pltpu
from jax.sharding import PartitionSpec as P


def dft_table(freq_index, length):
    sample_index = jnp.arange(length, dtype=jnp.int32)
    phases = freq_index[:, None] * sample_index[None, :] % length
    angles = phases.astype(jnp.float32) * jnp.float32(2.0 * math.pi / length)
    stacked = jnp.stack((jnp.cos(angles), -jnp.sin(angles)), axis=1)
    return stacked.reshape(freq_index.shape[0] * 2, length).astype(jnp.bfloat16)


def expand_map(block_map, receivers, points):
    row_span = receivers // block_map.shape[0]
    col_span = points // block_map.shape[1]
    return jnp.repeat(jnp.repeat(block_map, row_span, axis=0), col_span, axis=1).astype(
        jnp.bfloat16
    )


def transform(cos_table, records, length):
    spectrum = jnp.dot(cos_table, records.reshape(length, -1), preferred_element_type=jnp.float32)
    return (spectrum * (1.0 / math.sqrt(length))).astype(jnp.bfloat16)


def back_project(spectra, masked):
    swapped = jnp.stack((spectra[:, 1], -spectra[:, 0]), axis=1)
    blocks = jnp.stack((spectra, swapped), axis=1)
    return jnp.einsum("fcrx,focrs->fosx", masked, blocks, preferred_element_type=jnp.float32)


def body(traces, freq_index, block_map, green_rec, green_src):
    shards = lax.axis_size("freq")
    length = traces.shape[0] * shards
    receivers = traces.shape[1]
    shots = traces.shape[2]
    freqs = freq_index.shape[0]
    cos_table = dft_table(freq_index, length)
    masked = green_rec * expand_map(block_map, receivers, green_rec.shape[3])[None, None]
    regrouped = lax.all_to_all(traces, "freq", split_axis=2, concat_axis=0, tiled=True)
    spectrum = transform(cos_table, regrouped, length).reshape(freqs, 2, receivers, shots // shards)
    gathered = lax.all_to_all(spectrum, "freq", split_axis=0, concat_axis=3, tiled=True)
    back_field = back_project(gathered, masked)
    partial_image = jnp.sum(green_src.astype(jnp.float32) * back_field, axis=(0, 1, 2))
    return lax.psum_scatter(partial_image, "freq", scatter_dimension=0, tiled=True)


CORES = 2
ROWS = 2
PAIR = 2
LANES = 128
SUBLANES = 8
LEGS = 4


def chunks_of(half):
    first = (LANES, LANES) if half > 2 * LANES else (LANES,) * (half // LANES)
    sizes = list(first)
    while sum(sizes) < half:
        sizes.append(min(2 * LANES, half - sum(sizes)))
    return tuple((sum(sizes[:k]), size) for k, size in enumerate(sizes))


def seat(col, row, core):
    return (col * ROWS + row) * CORES + core


def remote(src, dst, send_sem, recv_sem, target):
    return pltpu.make_async_remote_copy(
        src_ref=src,
        dst_ref=dst,
        send_sem=send_sem,
        recv_sem=recv_sem,
        device_id={"freq": target},
        device_id_type=pl.DeviceIdType.MESH,
    )


def imaging_kernel(
    x_ref,
    fi_hbm,
    map_ref,
    green_ref,
    src_ref,
    out_ref,
    fi_ref,
    x_out,
    x_near,
    x_far,
    table,
    y_send,
    y_keep,
    y_recv,
    relay_send,
    relay_recv,
    cross_send,
    close_send,
    own_send,
    fin,
    green_v,
    src_v,
    map_v,
    mask_v,
    acc,
    i_send,
    i_recv,
    out_sem,
    near_sem,
    load_sem,
    green_sem,
    far_send,
    far_recv,
    ys_sem,
    yr_sem,
    rs_sem,
    rr_sem,
    cs_sem,
    ns_sem,
    os_sem,
    fin_sem,
    last_sem,
    is_sem,
    ir_sem,
    line_sem,
    pair_sem,
    row_sem,
):
    shards = i_send.shape[0]
    cols = shards // (ROWS * CORES)
    samples, folds, _, half = x_far.shape
    length = samples * shards
    steps = chunks_of(half)
    chunks = len(steps)
    freqs = fi_ref.shape[0]
    points = acc.shape[1]
    block = acc.shape[0]
    groups = 2 * folds
    depth = samples * SUBLANES
    bf16, f32 = jnp.bfloat16, jnp.float32

    me = lax.axis_index("freq")
    core = lax.rem(me, CORES)
    row = lax.rem(me // CORES, ROWS)
    col = me // (CORES * ROWS)
    near_col = col + 1 - 2 * lax.rem(col, PAIR)
    cross_col = lax.rem(col + PAIR, cols)
    far_col = lax.rem(near_col + PAIR, cols)
    leg_cols = (far_col, cross_col, near_col, col)
    mate = seat(col, row, 1 - core)
    across = seat(col, 1 - row, core)

    barrier = pltpu.get_barrier_semaphore()

    def tell(sem, target):
        pl.semaphore_signal(
            sem, inc=1, device_id={"freq": target}, device_id_type=pl.DeviceIdType.MESH
        )

    def tell_line(sem):
        @pl.when(col > 0)
        def _():
            tell(sem, seat(col - 1, row, core))

        @pl.when(col < cols - 1)
        def _():
            tell(sem, seat(col + 1, row, core))

    beside = jnp.minimum(col, 1) + jnp.minimum(cols - 1 - col, 1)

    def at(k):
        return pl.ds(*steps[k])

    def lanes(core_at, k):
        return pl.ds(pl.multiple_of(core_at * half + steps[k][0], LANES), steps[k][1])

    def out_load(k):
        return pltpu.make_async_copy(
            x_ref.at[:, :, :, lanes(1 - core, k)], x_out.at[:, :, :, at(k)], out_sem.at[k]
        )

    def near_load(k):
        return pltpu.make_async_copy(
            x_ref.at[:, :, :, lanes(core, k)], x_near.at[:, :, :, at(k)], near_sem.at[k]
        )

    def far_copy(k):
        return remote(
            x_out.at[:, :, :, at(k)], x_far.at[:, :, :, at(k)], far_send, far_recv.at[k], mate
        )

    def green_load(k, side, part):
        core_at = core if side == 0 else 1 - core
        start, size = steps[k]
        place = CORES * 2 * start + (2 * side + part) * size
        origin = pl.multiple_of(part * CORES * half + core_at * half + start, LANES)
        return pltpu.make_async_copy(
            green_ref.at[pl.ds(origin, size), :], green_v.at[pl.ds(place, size), :], green_sem.at[k]
        )

    fi_load = pltpu.make_async_copy(fi_hbm, fi_ref, load_sem.at[0])
    map_load = pltpu.make_async_copy(map_ref, map_v, load_sem.at[1])
    src_load = pltpu.make_async_copy(src_ref, src_v, load_sem.at[2])
    fi_load.start()
    for k in range(chunks):
        out_load(k).start()
    tell(barrier, mate)
    tell(barrier, across)
    tell_line(barrier)
    for k in range(chunks):
        near_load(k).start()

    table_rows = 2 * freqs
    span = CORES * samples
    line = lax.broadcasted_iota(jnp.int32, (table_rows, span), 0)
    column = lax.broadcasted_iota(jnp.int32, (table_rows, span), 1)
    wide = span * SUBLANES
    spread = lax.broadcasted_iota(jnp.int32, (span, wide), 1) // SUBLANES == lax.broadcasted_iota(
        jnp.int32, (span, wide), 0
    )
    fi_load.wait()
    bins = jnp.zeros((table_rows, span), jnp.int32)
    for side in range(ROWS):
        for leg in range(LEGS):
            for k in range(CORES):
                to_row = 1 - row if side == 0 else row
                place = (side * LEGS + leg) * CORES + k
                bins = jnp.where(line // 2 == place, fi_ref[seat(leg_cols[leg], to_row, k)], bins)
    time = jnp.where(column < samples, me * samples + column, (mate - 1) * samples + column)
    angles = lax.rem(bins * time, length).astype(f32) * f32(2.0 * math.pi / length)
    small = jnp.where(line % 2 == 0, jnp.cos(angles), -jnp.sin(angles)).astype(bf16)
    stretched = jnp.dot(small, jnp.where(spread, 1.0, 0.0).astype(bf16), preferred_element_type=f32)
    same_shot = lax.broadcasted_iota(jnp.int32, (SUBLANES, wide), 1) % SUBLANES == (
        lax.broadcasted_iota(jnp.int32, (SUBLANES, wide), 0)
    )
    for r in range(table_rows):
        spread_row = jnp.broadcast_to(stretched[r : r + 1, :], (SUBLANES, wide))
        table[r * SUBLANES : (r + 1) * SUBLANES, :] = jnp.where(same_shot, spread_row, 0.0).astype(
            bf16
        )

    pl.semaphore_wait(barrier, 2 + beside)
    for k in range(chunks):
        out_load(k).wait()
        far_copy(k).start()
    map_load.start()
    src_load.start()
    for k in range(chunks):
        for side in range(CORES):
            for part in range(2):
                green_load(k, side, part).start()
    tell_line(line_sem.at[0])

    rows = LEGS * CORES * 2 * SUBLANES

    def partial(side, fold, k):
        size = steps[k][1]
        total = None
        for part, ref in enumerate((x_near, x_far)):
            seen = ref[:, fold, :, at(k)].reshape(depth, size)
            weights = table[side * rows : (side + 1) * rows, part * depth : (part + 1) * depth]
            term = jnp.dot(weights, seen, preferred_element_type=f32)
            total = term if total is None else total + term
        return total

    def fill(ref, side, k):
        for fold in range(folds):
            total = partial(side, fold, k)
            for leg in range(LEGS):
                for line_at in range(2 * CORES):
                    first = (leg * 2 * CORES + line_at) * SUBLANES
                    ref[leg, line_at * folds + fold, :, at(k)] = total[
                        first : first + SUBLANES
                    ].astype(ref.dtype)

    def y_copy(leg, k):
        return remote(
            y_send.at[leg, :, :, at(k)],
            y_recv.at[leg, :, :, at(k)],
            ys_sem,
            yr_sem.at[leg, k],
            across,
        )

    def pick(core_at):
        return pl.ds(core_at * groups, groups)

    def deliver(src_ref_at, kind, k, sem, arrived, to_col, to_row):
        for side in range(CORES):
            to_core = core if side == 0 else 1 - core
            remote(
                src_ref_at(to_core),
                fin.at[kind * CORES + side, :, :, at(k)],
                sem,
                arrived,
                seat(to_col, to_row, to_core),
            ).start()

    def last_copies(k):
        deliver(
            lambda c: y_send.at[LEGS - 1, pick(c), :, at(k)], 0, k, ys_sem, last_sem.at[k], col, 1 - row
        )

    def own_copy(k):
        return remote(
            own_send.at[:, :, at(k)], fin.at[3 * CORES, :, :, at(k)], os_sem, fin_sem.at[k], mate
        )

    def send_partial(k):
        near_load(k).wait()
        far_copy(k).wait_recv()
        fill(y_send, 0, k)
        y_copy(0, k).start()
        y_copy(1, k).start()

    def keep_partial(k):
        fill(y_keep, 1, k)
        own_send[:, :, at(k)] = y_keep[LEGS - 1, pick(1 - core), :, at(k)].astype(bf16)
        own_copy(k).start()

    def relay_copy(k):
        return remote(
            relay_send.at[:, :, at(k)],
            relay_recv.at[:, :, at(k)],
            rs_sem,
            rr_sem.at[k],
            seat(near_col, row, core),
        )

    def joined(leg, k):
        y_copy(leg, k).wait_recv()
        return y_keep[leg, :, :, at(k)] + y_recv[leg, :, :, at(k)].astype(f32)

    def pass_on(k):
        relay_send[:, :, at(k)] = joined(0, k).astype(bf16)
        relay_copy(k).start()

    def cross(k):
        total = joined(1, k)
        relay_copy(k).wait_recv()
        cross_send[:, :, at(k)] = (total + relay_recv[:, :, at(k)].astype(f32)).astype(bf16)
        deliver(lambda c: cross_send.at[pick(c), :, at(k)], 2, k, cs_sem, fin_sem.at[k], cross_col, row)

    def close(k):
        close_send[:, :, at(k)] = joined(2, k).astype(bf16)
        deliver(lambda c: close_send.at[pick(c), :, at(k)], 1, k, ns_sem, fin_sem.at[k], near_col, row)

    tiles = map_v.shape[1]

    def make_mask():
        map_load.wait()
        in_tile = lax.broadcasted_iota(jnp.int32, (tiles, points), 1) // (
            points // tiles
        ) == lax.broadcasted_iota(jnp.int32, (tiles, points), 0)
        mask_v[...] = jnp.dot(
            map_v[...].astype(f32).astype(bf16),
            jnp.where(in_tile, 1.0, 0.0).astype(bf16),
            preferred_element_type=f32,
        )
        acc[...] = jnp.zeros_like(acc)

    deep = CORES * half // map_v.shape[0]

    def mask_chunk(k):
        start, size = steps[k]
        whole = green_v.at[pl.ds(CORES * 2 * start, CORES * 2 * size), :]
        pltpu.make_async_copy(whole, whole, green_sem.at[k]).wait()
        for side in range(CORES):
            core_at = core if side == 0 else 1 - core
            for i in range(size // deep):
                seen = mask_v[pl.ds((core_at * half + start) // deep + i, 1), :]
                seen = jnp.broadcast_to(seen, (deep, points)).astype(bf16)
                for part in range(2):
                    place = CORES * 2 * start + (2 * side + part) * size + i * deep
                    green_v[place : place + deep, :] = green_v[place : place + deep, :] * seen

    def consume(k):
        start, size = steps[k]
        wait_fin(k)
        own = y_keep[LEGS - 1, pick(core), :, at(k)]
        sums = []
        for side in range(CORES):
            total = own if side == 0 else fin[3 * CORES, :, :, at(k)].astype(f32)
            sums.append(
                total
                + fin[CORES + side, :, :, at(k)].astype(f32)
                + fin[2 * CORES + side, :, :, at(k)].astype(f32)
            )
        wait_last(k)
        parts = []
        for side in range(CORES):
            total = sums[side] + fin[side, :, :, at(k)].astype(f32)
            spectrum = total.reshape(block, size) * f32(1.0 / math.sqrt(length))
            turned = jnp.concatenate((spectrum[block // 2 :], -spectrum[: block // 2]), axis=0)
            parts += [spectrum.astype(bf16), turned.astype(bf16)]
        acc[...] += jnp.dot(
            jnp.concatenate(parts, axis=1),
            green_v[CORES * 2 * start : CORES * 2 * (start + size), :],
            preferred_element_type=f32,
        )

    def wait_fin(k):
        five = fin.at[pl.ds(CORES, 2 * CORES + 1), :, :, at(k)]
        pltpu.make_async_copy(five, five, fin_sem.at[k]).wait()

    def wait_last(k):
        two = fin.at[pl.ds(0, CORES), :, :, at(k)]
        pltpu.make_async_copy(two, two, last_sem.at[k]).wait()

    for k in range(chunks):
        send_partial(k)
        if k == 1:
            pl.semaphore_wait(line_sem.at[0], beside)
            tell_line(line_sem.at[1])
        if k == 2:
            pl.semaphore_wait(line_sem.at[1], beside)
            tell(pair_sem, mate)
    for k in range(chunks):
        y_copy(2, k).start()
    keep_partial(0)
    pl.semaphore_wait(pair_sem, 1)
    tell(row_sem, across)
    for k in range(chunks):
        last_copies(k)
    keep_partial(1)

    events = []
    clock = 0.0
    unit = 0.7 / (2 * LANES)
    for k in range(chunks):
        clock += steps[k][1] * unit
        events.append((clock, 0, lambda k=k: pass_on(k)))
        ready = clock + 2.2 + steps[k][1] * unit
        clock += steps[k][1] * unit
        events.append((max(clock, ready), 1, lambda k=k: cross(k)))
    for k in range(chunks):
        clock += steps[k][1] * unit
        events.append((clock, 2, lambda k=k: close(k)))
    for k in range(chunks):
        clock += steps[k][1] * unit
        events.append((clock, 4, lambda k=k: consume(k)))
    for k in range(2, chunks):
        events.append((0.2 + 1.4 * (k - 2), 3, lambda k=k: keep_partial(k)))
    events.append((1.0, 5, make_mask))
    for k in range(chunks):
        events.append((3.0 + 0.9 * k, 6, lambda k=k: mask_chunk(k)))
    for _, _, run in sorted(events, key=lambda e: e[:2]):
        run()

    src_load.wait()
    product = src_v[...].astype(f32) * acc[...]
    folded = product[0:SUBLANES]
    for first in range(SUBLANES, block, SUBLANES):
        folded = folded + product[first : first + SUBLANES]
    flat = jnp.broadcast_to(jnp.sum(folded, axis=0, keepdims=True), (SUBLANES, points))
    each = points // shards
    for d in range(shards):
        i_send[d] = pltpu.roll(flat, (points - d * each) % points, 1)[0:1, :LANES]

    def i_copy(step):
        to = lax.rem(me + step, shards)
        return remote(i_send.at[to], i_recv.at[step], is_sem, ir_sem, to)

    pl.semaphore_wait(row_sem, 1)
    for step in range(1, shards):
        i_copy(step).start()
    total = i_send[me]
    others = i_recv.at[pl.ds(1, shards - 1)]
    pltpu.make_async_copy(others, others, ir_sem).wait()
    for step in range(1, shards):
        total = total + i_recv[step]
    out_ref[...] = total

    for sent, sem in (
        (x_out, far_send),
        (y_send, ys_sem),
        (relay_send, rs_sem),
        (cross_send, cs_sem),
        (close_send, ns_sem),
        (own_send, os_sem),
        (others, is_sem),
    ):
        pltpu.make_async_copy(sent, sent, sem).wait()


def fused_body(traces, freq_index, block_map, green_rec, green_src):
    shards = lax.axis_size("freq")
    samples, receivers, shots = traces.shape
    points = green_rec.shape[3]
    freqs = freq_index.shape[0]
    half = receivers // CORES
    chunks = len(chunks_of(half))
    folds = shots // SUBLANES
    records = jnp.transpose(traces, (0, 2, 1)).reshape(samples, folds, SUBLANES, receivers)
    green = green_rec.reshape(2 * receivers, points)
    sources = green_src.reshape(2 * shots, points)
    block = 2 * shots
    groups = 2 * folds
    bf16, f32 = jnp.bfloat16, jnp.float32
    dma = pltpu.SemaphoreType.DMA
    regular = pltpu.SemaphoreType.REGULAR
    outside = pl.BlockSpec(memory_space=pltpu.HBM)
    piece = (CORES * groups, SUBLANES, half)
    image = pl.pallas_call(
        imaging_kernel,
        out_shape=jax.ShapeDtypeStruct((1, LANES), f32),
        in_specs=[outside] * 5,
        out_specs=pl.BlockSpec(memory_space=pltpu.VMEM),
        scratch_shapes=[
            pltpu.SMEM(freq_index.shape, jnp.int32),
            pltpu.VMEM((samples, folds, SUBLANES, half), bf16),
            pltpu.VMEM((samples, folds, SUBLANES, half), bf16),
            pltpu.VMEM((samples, folds, SUBLANES, half), bf16),
            pltpu.VMEM((2 * freqs * SUBLANES, CORES * samples * SUBLANES), bf16),
            pltpu.VMEM((LEGS,) + piece, bf16),
            pltpu.VMEM((LEGS,) + piece, f32),
            pltpu.VMEM((LEGS - 1,) + piece, bf16),
            pltpu.VMEM(piece, bf16),
            pltpu.VMEM(piece, bf16),
            pltpu.VMEM(piece, bf16),
            pltpu.VMEM(piece, bf16),
            pltpu.VMEM((groups, SUBLANES, half), bf16),
            pltpu.VMEM((3 * CORES + 1, groups, SUBLANES, half), bf16),
            pltpu.VMEM((2 * receivers, points), bf16),
            pltpu.VMEM((block, points), bf16),
            pltpu.VMEM(block_map.shape, jnp.int32),
            pltpu.VMEM((block_map.shape[0], points), f32),
            pltpu.VMEM((block, points), f32),
            pltpu.VMEM((shards, 1, LANES), f32),
            pltpu.VMEM((shards, 1, LANES), f32),
            dma((chunks,)),
            dma((chunks,)),
            dma((3,)),
            dma((chunks,)),
            dma,
            dma((chunks,)),
            dma,
            dma((LEGS - 1, chunks)),
            dma,
            dma((chunks,)),
            dma,
            dma,
            dma,
            dma((chunks,)),
            dma((chunks,)),
            dma,
            dma,
            regular((PAIR,)),
            regular,
            regular,
        ],
        compiler_params=pltpu.CompilerParams(
            collective_id=0, has_side_effects=True, vmem_limit_bytes=48 * 1024 * 1024
        ),
    )(
        *(
            pltpu.with_memory_space_constraint(array, pltpu.HBM)
            for array in (records, freq_index, block_map, green, sources)
        )
    )
    return image[0, : points // shards]


def moves_less(traces, freq_index, block_map, green_rec):
    shards = lax.axis_size("freq")
    samples, receivers, shots = traces.shape
    freqs = freq_index.shape[0]
    return (
        2 * freqs <= samples
        and freqs == shards
        and shards == 2 * PAIR * ROWS * CORES
        and shots % SUBLANES == 0
        and receivers % (CORES * LANES) == 0
        and LANES % (receivers // block_map.shape[0]) == 0
        and green_rec.shape[3] % LANES == 0
        and green_rec.shape[3] // shards <= LANES
    )


def chosen_body(traces, freq_index, block_map, green_rec, green_src):
    fused = moves_less(traces, freq_index, block_map, green_rec)
    return (fused_body if fused else body)(traces, freq_index, block_map, green_rec, green_src)


def solution(mesh):
    in_specs = (
        P("freq", None, "groups"),
        P(),
        P(),
        P("freq", None, None, "groups"),
        P("freq", None, None, "groups"),
    )
    out_specs = P(("groups", "freq"))
    return jax.shard_map(chosen_body, mesh=mesh, in_specs=in_specs, out_specs=out_specs, check_vma=False)
```

```python
import math

import jax
import jax.numpy as jnp
from jax import lax
from jax.experimental import pallas as pl
from jax.experimental.pallas import tpu as pltpu
from jax.sharding import PartitionSpec as P


def dft_table(freq_index, length):
    sample_index = jnp.arange(length, dtype=jnp.int32)
    phases = freq_index[:, None] * sample_index[None, :] % length
    angles = phases.astype(jnp.float32) * jnp.float32(2.0 * math.pi / length)
    stacked = jnp.stack((jnp.cos(angles), -jnp.sin(angles)), axis=1)
    return stacked.reshape(freq_index.shape[0] * 2, length).astype(jnp.bfloat16)


def expand_map(block_map, receivers, points):
    row_span = receivers // block_map.shape[0]
    col_span = points // block_map.shape[1]
    return jnp.repeat(jnp.repeat(block_map, row_span, axis=0), col_span, axis=1).astype(
        jnp.bfloat16
    )


def transform(cos_table, records, length):
    spectrum = jnp.dot(cos_table, records.reshape(length, -1), preferred_element_type=jnp.float32)
    return (spectrum * (1.0 / math.sqrt(length))).astype(jnp.bfloat16)


def back_project(spectra, masked):
    swapped = jnp.stack((spectra[:, 1], -spectra[:, 0]), axis=1)
    blocks = jnp.stack((spectra, swapped), axis=1)
    return jnp.einsum("fcrx,focrs->fosx", masked, blocks, preferred_element_type=jnp.float32)


def body(traces, freq_index, block_map, green_rec, green_src):
    shards = lax.axis_size("freq")
    length = traces.shape[0] * shards
    receivers = traces.shape[1]
    shots = traces.shape[2]
    freqs = freq_index.shape[0]
    cos_table = dft_table(freq_index, length)
    masked = green_rec * expand_map(block_map, receivers, green_rec.shape[3])[None, None]
    regrouped = lax.all_to_all(traces, "freq", split_axis=2, concat_axis=0, tiled=True)
    spectrum = transform(cos_table, regrouped, length).reshape(freqs, 2, receivers, shots // shards)
    gathered = lax.all_to_all(spectrum, "freq", split_axis=0, concat_axis=3, tiled=True)
    back_field = back_project(gathered, masked)
    partial_image = jnp.sum(green_src.astype(jnp.float32) * back_field, axis=(0, 1, 2))
    return lax.psum_scatter(partial_image, "freq", scatter_dimension=0, tiled=True)


CORES = 2
ROWS = 2
PAIR = 2
LANES = 128
SUBLANES = 8
LEGS = 4
DIRECT = 1


def chunks_of(half):
    sizes = [LANES, LANES]
    while sum(sizes) < half:
        sizes.append(min(2 * LANES, half - sum(sizes)))
    return tuple((sum(sizes[:k]), size) for k, size in enumerate(sizes))


def seat(col, row, core):
    return (col * ROWS + row) * CORES + core


def remote(src, dst, send_sem, recv_sem, target):
    return pltpu.make_async_remote_copy(
        src_ref=src,
        dst_ref=dst,
        send_sem=send_sem,
        recv_sem=recv_sem,
        device_id={"freq": target},
        device_id_type=pl.DeviceIdType.MESH,
    )


def imaging_kernel(
    x_ref,
    fi_hbm,
    map_ref,
    green_ref,
    src_ref,
    out_ref,
    fi_ref,
    x_out,
    x_near,
    x_far,
    table,
    y_send,
    y_keep,
    y_recv,
    relay_send,
    relay_recv,
    cross_send,
    close_send,
    own_send,
    fin,
    d_send,
    d_keep,
    d_recv,
    d_sum,
    d_own,
    d_fin,
    green_v,
    src_v,
    map_v,
    mask_v,
    acc,
    i_send,
    i_recv,
    out_sem,
    near_sem,
    load_sem,
    green_sem,
    far_send,
    far_recv,
    ys_sem,
    yr_sem,
    rs_sem,
    rr_sem,
    cs_sem,
    ns_sem,
    os_sem,
    fin_sem,
    last_sem,
    ds_sem,
    dr_sem,
    dp_sem,
    df_sem,
    is_sem,
    ir_sem,
    line_sem,
    pair_sem,
    row_sem,
):
    shards = i_send.shape[0]
    cols = shards // (ROWS * CORES)
    samples, folds, _, half = x_far.shape
    length = samples * shards
    steps = chunks_of(half)
    chunks = len(steps)
    folded = [k for k in range(chunks) if k != DIRECT]
    freqs = fi_ref.shape[0]
    points = acc.shape[1]
    block = acc.shape[0]
    groups = 2 * folds
    depth = samples * SUBLANES
    bf16, f32 = jnp.bfloat16, jnp.float32

    me = lax.axis_index("freq")
    core = lax.rem(me, CORES)
    row = lax.rem(me // CORES, ROWS)
    col = me // (CORES * ROWS)
    near_col = col + 1 - 2 * lax.rem(col, PAIR)
    cross_col = lax.rem(col + PAIR, cols)
    far_col = lax.rem(near_col + PAIR, cols)
    leg_cols = (far_col, cross_col, near_col, col)
    mate = seat(col, row, 1 - core)
    across = seat(col, 1 - row, core)

    barrier = pltpu.get_barrier_semaphore()

    def tell(sem, target):
        pl.semaphore_signal(
            sem, inc=1, device_id={"freq": target}, device_id_type=pl.DeviceIdType.MESH
        )

    def tell_line(sem):
        @pl.when(col > 0)
        def _():
            tell(sem, seat(col - 1, row, core))

        @pl.when(col < cols - 1)
        def _():
            tell(sem, seat(col + 1, row, core))

    beside = jnp.minimum(col, 1) + jnp.minimum(cols - 1 - col, 1)

    def at(k):
        return pl.ds(*steps[k])

    def lanes(core_at, k):
        return pl.ds(pl.multiple_of(core_at * half + steps[k][0], LANES), steps[k][1])

    def out_load(k):
        return pltpu.make_async_copy(
            x_ref.at[:, :, :, lanes(1 - core, k)], x_out.at[:, :, :, at(k)], out_sem.at[k]
        )

    def near_load(k):
        return pltpu.make_async_copy(
            x_ref.at[:, :, :, lanes(core, k)], x_near.at[:, :, :, at(k)], near_sem.at[k]
        )

    def far_copy(k):
        return remote(
            x_out.at[:, :, :, at(k)], x_far.at[:, :, :, at(k)], far_send, far_recv.at[k], mate
        )

    def green_load(k, side, part):
        core_at = core if side == 0 else 1 - core
        start, size = steps[k]
        place = CORES * 2 * start + (2 * side + part) * size
        origin = pl.multiple_of(part * CORES * half + core_at * half + start, LANES)
        return pltpu.make_async_copy(
            green_ref.at[pl.ds(origin, size), :], green_v.at[pl.ds(place, size), :], green_sem
        )

    fi_load = pltpu.make_async_copy(fi_hbm, fi_ref, load_sem.at[0])
    map_load = pltpu.make_async_copy(map_ref, map_v, load_sem.at[1])
    src_load = pltpu.make_async_copy(src_ref, src_v, load_sem.at[2])
    fi_load.start()
    order = folded[:2] + [DIRECT] + folded[2:]
    out_load(order[0]).start()
    for k, later in zip(order, order[1:]):
        out_load(later).start()
        near_load(k).start()
    near_load(order[-1]).start()
    tell(barrier, mate)
    tell(barrier, across)
    tell_line(barrier)

    table_rows = 2 * freqs
    span = CORES * samples
    line = lax.broadcasted_iota(jnp.int32, (table_rows, span), 0)
    column = lax.broadcasted_iota(jnp.int32, (table_rows, span), 1)
    wide = span * SUBLANES
    spread = lax.broadcasted_iota(jnp.int32, (span, wide), 1) // SUBLANES == lax.broadcasted_iota(
        jnp.int32, (span, wide), 0
    )
    pl.semaphore_wait(barrier, 2 + beside)
    out_load(order[0]).wait()
    far_copy(order[0]).start()
    fi_load.wait()
    bins = jnp.zeros((table_rows, span), jnp.int32)
    for side in range(ROWS):
        for leg in range(LEGS):
            for k in range(CORES):
                to_row = 1 - row if side == 0 else row
                place = (side * LEGS + leg) * CORES + k
                bins = jnp.where(line // 2 == place, fi_ref[seat(leg_cols[leg], to_row, k)], bins)
    time = jnp.where(column < samples, me * samples + column, (mate - 1) * samples + column)
    angles = lax.rem(bins * time, length).astype(f32) * f32(2.0 * math.pi / length)
    small = jnp.where(line % 2 == 0, jnp.cos(angles), -jnp.sin(angles)).astype(bf16)
    stretched = jnp.dot(small, jnp.where(spread, 1.0, 0.0).astype(bf16), preferred_element_type=f32)
    same_shot = lax.broadcasted_iota(jnp.int32, (SUBLANES, wide), 1) % SUBLANES == (
        lax.broadcasted_iota(jnp.int32, (SUBLANES, wide), 0)
    )
    for r in range(table_rows):
        spread_row = jnp.broadcast_to(stretched[r : r + 1, :], (SUBLANES, wide))
        table[r * SUBLANES : (r + 1) * SUBLANES, :] = jnp.where(same_shot, spread_row, 0.0).astype(
            bf16
        )

    tell_line(line_sem.at[0])

    def hand_over(k):
        out_load(k).wait()
        far_copy(k).start()

    hand_over(order[1])
    hand_over(order[2])
    map_load.start()
    src_load.start()

    def start_green(k):
        for side in range(CORES):
            for part in range(2):
                green_load(k, side, part).start()

    rows = LEGS * CORES * 2 * SUBLANES

    def partial(side, fold, k):
        size = steps[k][1]
        total = None
        for part, ref in enumerate((x_near, x_far)):
            seen = ref[:, fold, :, at(k)].reshape(depth, size)
            weights = table[side * rows : (side + 1) * rows, part * depth : (part + 1) * depth]
            term = jnp.dot(weights, seen, preferred_element_type=f32)
            total = term if total is None else total + term
        return total

    def fill(ref, side, k):
        for fold in range(folds):
            total = partial(side, fold, k)
            for leg in range(LEGS):
                for line_at in range(2 * CORES):
                    first = (leg * 2 * CORES + line_at) * SUBLANES
                    ref[leg, line_at * folds + fold, :, at(k)] = total[
                        first : first + SUBLANES
                    ].astype(ref.dtype)

    def y_copy(leg, k):
        return remote(
            y_send.at[leg, :, :, at(k)],
            y_recv.at[leg, :, :, at(k)],
            ys_sem,
            yr_sem.at[leg, k],
            across,
        )

    def pick(core_at):
        return pl.ds(core_at * groups, groups)

    def deliver(src_ref_at, kind, k, sem, arrived, to_col, to_row):
        for side in range(CORES):
            to_core = core if side == 0 else 1 - core
            remote(
                src_ref_at(to_core),
                fin.at[kind * CORES + side, :, :, at(k)],
                sem,
                arrived,
                seat(to_col, to_row, to_core),
            ).start()

    def last_copies(k):
        deliver(
            lambda c: y_send.at[LEGS - 1, pick(c), :, at(k)], 0, k, ys_sem, last_sem.at[k], col, 1 - row
        )

    def own_copy(k):
        return remote(
            own_send.at[:, :, at(k)], fin.at[3 * CORES, :, :, at(k)], os_sem, fin_sem.at[k], mate
        )

    def send_partial(k):
        near_load(k).wait()
        far_copy(k).wait_recv()
        fill(y_send, 0, k)
        y_copy(0, k).start()

    def keep_partial(k):
        fill(y_keep, 1, k)
        own_send[:, :, at(k)] = y_keep[LEGS - 1, pick(1 - core), :, at(k)].astype(bf16)
        own_copy(k).start()

    def relay_copy(k):
        return remote(
            relay_send.at[:, :, at(k)],
            relay_recv.at[:, :, at(k)],
            rs_sem,
            rr_sem.at[k],
            seat(near_col, row, core),
        )

    def joined(leg, k):
        y_copy(leg, k).wait_recv()
        return y_keep[leg, :, :, at(k)] + y_recv[leg, :, :, at(k)].astype(f32)

    def pass_on(k):
        relay_send[:, :, at(k)] = joined(0, k).astype(bf16)
        relay_copy(k).start()

    def cross(k):
        total = joined(1, k)
        relay_copy(k).wait_recv()
        cross_send[:, :, at(k)] = (total + relay_recv[:, :, at(k)].astype(f32)).astype(bf16)
        deliver(lambda c: cross_send.at[pick(c), :, at(k)], 2, k, cs_sem, fin_sem.at[k], cross_col, row)

    def close(k):
        close_send[:, :, at(k)] = joined(2, k).astype(bf16)
        deliver(lambda c: close_send.at[pick(c), :, at(k)], 1, k, ns_sem, fin_sem.at[k], near_col, row)

    def direct_copy(leg):
        return remote(
            d_send.at[leg], d_recv.at[leg], ds_sem, dr_sem, seat(leg_cols[leg], row, core)
        )

    def send_direct():
        near_load(DIRECT).wait()
        far_copy(DIRECT).wait_recv()
        for side in range(ROWS):
            for fold in range(folds):
                total = partial(side, fold, DIRECT)
                for leg in range(LEGS):
                    for line_at in range(2 * CORES):
                        first = (leg * 2 * CORES + line_at) * SUBLANES
                        place = (side * 2 * CORES + line_at) * folds + fold
                        value = total[first : first + SUBLANES]
                        if leg < LEGS - 1:
                            d_send[leg, place] = value.astype(bf16)
                        else:
                            d_keep[place] = value
        for leg in range(LEGS - 1):
            direct_copy(leg).start()

    def join_direct():
        pltpu.make_async_copy(d_recv, d_recv, dr_sem).wait()
        total = d_keep[...]
        for leg in range(LEGS - 1):
            total = total + d_recv[leg].astype(f32)
        d_keep[...] = total
        d_sum[...] = total.astype(bf16)
        d_own[...] = d_keep[pl.ds((CORES + core) * groups, groups)]
        for slot, side, to_core, target in (
            (1, 0, core, across),
            (2, 0, 1 - core, seat(col, 1 - row, 1 - core)),
            (0, 1, 1 - core, mate),
        ):
            remote(
                d_sum.at[pl.ds((side * CORES + to_core) * groups, groups)],
                d_fin.at[slot],
                dp_sem,
                df_sem,
                target,
            ).start()

    tiles = map_v.shape[1]

    def make_mask():
        map_load.wait()
        pltpu.make_async_copy(green_v, green_v, green_sem).wait()
        in_tile = lax.broadcasted_iota(jnp.int32, (tiles, points), 1) // (
            points // tiles
        ) == lax.broadcasted_iota(jnp.int32, (tiles, points), 0)
        mask_v[...] = jnp.dot(
            map_v[...].astype(f32).astype(bf16),
            jnp.where(in_tile, 1.0, 0.0).astype(bf16),
            preferred_element_type=f32,
        )
        acc[...] = jnp.zeros_like(acc)

    deep = CORES * half // map_v.shape[0]

    def mask_chunk(k):
        start, size = steps[k]
        for side in range(CORES):
            core_at = core if side == 0 else 1 - core
            for i in range(size // deep):
                seen = mask_v[pl.ds((core_at * half + start) // deep + i, 1), :]
                seen = jnp.broadcast_to(seen, (deep, points)).astype(bf16)
                for part in range(2):
                    place = CORES * 2 * start + (2 * side + part) * size + i * deep
                    green_v[place : place + deep, :] = green_v[place : place + deep, :] * seen

    def use(k, totals):
        start, size = steps[k]
        parts = []
        for total in totals:
            spectrum = total.reshape(block, size) * f32(1.0 / math.sqrt(length))
            turned = jnp.concatenate((spectrum[block // 2 :], -spectrum[: block // 2]), axis=0)
            parts += [spectrum.astype(bf16), turned.astype(bf16)]
        acc[...] += jnp.dot(
            jnp.concatenate(parts, axis=1),
            green_v[CORES * 2 * start : CORES * 2 * (start + size), :],
            preferred_element_type=f32,
        )

    def consume(k):
        wait_fin(k)
        own = y_keep[LEGS - 1, pick(core), :, at(k)]
        sums = []
        for side in range(CORES):
            total = own if side == 0 else fin[3 * CORES, :, :, at(k)].astype(f32)
            sums.append(
                total
                + fin[CORES + side, :, :, at(k)].astype(f32)
                + fin[2 * CORES + side, :, :, at(k)].astype(f32)
            )
        wait_last(k)
        use(k, [sums[side] + fin[side, :, :, at(k)].astype(f32) for side in range(CORES)])

    def consume_direct():
        pltpu.make_async_copy(d_fin, d_fin, df_sem).wait()
        use(
            DIRECT,
            [
                d_own[...] + d_fin[1].astype(f32),
                d_fin[0].astype(f32) + d_fin[2].astype(f32),
            ],
        )

    def wait_fin(k):
        five = fin.at[pl.ds(CORES, 2 * CORES + 1), :, :, at(k)]
        pltpu.make_async_copy(five, five, fin_sem.at[k]).wait()

    def wait_last(k):
        two = fin.at[pl.ds(0, CORES), :, :, at(k)]
        pltpu.make_async_copy(two, two, last_sem.at[k]).wait()

    send_partial(order[0])
    hand_over(order[3])
    pl.semaphore_wait(line_sem.at[0], beside)
    tell_line(line_sem.at[1])
    send_partial(order[1])
    for k in order[4:]:
        hand_over(k)
    pl.semaphore_wait(line_sem.at[1], beside)
    tell(pair_sem, mate)
    for k in range(chunks):
        start_green(k)
    send_direct()
    for at_fold, k in enumerate(folded[2:]):
        send_partial(k)
        keep_partial(folded[at_fold])
    for leg in (1, 2):
        for k in folded:
            y_copy(leg, k).start()
    pl.semaphore_wait(pair_sem, 1)
    tell(row_sem, across)

    def send_last():
        join_direct()
        for k in folded:
            last_copies(k)

    wire = 0.7 / (2 * LANES)
    hop = 2.6
    events = [(4.0, 5, make_mask), (4.3, 7, send_last)]
    for place, k in enumerate(folded[len(folded) - 2 :]):
        events.append((0.8 + 0.7 * place, 8, lambda k=k: keep_partial(k)))
    clock = mid = 0.0
    handed = {}
    for leg in range(LEGS):
        for k in folded:
            span = steps[k][1] * wire
            clock += span
            if leg == 0:
                events.append((clock, leg, lambda k=k: pass_on(k)))
                handed[k] = clock + span + hop
            elif leg == 1:
                ready = max(clock, handed[k])
                mid = max(mid, ready) + 2 * span
                handed[k] = mid + hop + 0.5
                events.append((ready, leg, lambda k=k: cross(k)))
            elif leg == 2:
                handed[k] = max(handed[k], clock + span + hop)
                events.append((clock, leg, lambda k=k: close(k)))
            else:
                events.append((max(clock, handed[k]), leg, lambda k=k: consume(k)))
    events.append((8.6, 9, consume_direct))
    for k in range(chunks):
        events.append((5.0 + 0.6 * k, 6, lambda k=k: mask_chunk(k)))
    for _, _, run in sorted(events, key=lambda e: e[:2]):
        run()

    src_load.wait()
    product = src_v[...].astype(f32) * acc[...]
    folded = product[0:SUBLANES]
    for first in range(SUBLANES, block, SUBLANES):
        folded = folded + product[first : first + SUBLANES]
    flat = jnp.broadcast_to(jnp.sum(folded, axis=0, keepdims=True), (SUBLANES, points))
    each = points // shards
    for d in range(shards):
        i_send[d] = pltpu.roll(flat, (points - d * each) % points, 1)[0:1, :LANES]

    def i_copy(step):
        to = lax.rem(me + step, shards)
        return remote(i_send.at[to], i_recv.at[step], is_sem, ir_sem, to)

    pl.semaphore_wait(row_sem, 1)
    for step in range(1, shards):
        i_copy(step).start()
    total = i_send[me]
    others = i_recv.at[pl.ds(1, shards - 1)]
    rest = pl.ds(0, half - steps[DIRECT][1])
    for sent, sem in (
        (x_out, far_send),
        (y_send.at[:, :, :, rest], ys_sem),
        (relay_send.at[:, :, rest], rs_sem),
        (cross_send.at[:, :, rest], cs_sem),
        (close_send.at[:, :, rest], ns_sem),
        (own_send.at[:, :, rest], os_sem),
        (d_send, ds_sem),
        (d_fin, dp_sem),
    ):
        pltpu.make_async_copy(sent, sent, sem).wait()
    pltpu.make_async_copy(others, others, ir_sem).wait()
    for step in range(1, shards):
        total = total + i_recv[step]
    out_ref[...] = total
    pltpu.make_async_copy(others, others, is_sem).wait()


def fused_body(traces, freq_index, block_map, green_rec, green_src):
    shards = lax.axis_size("freq")
    samples, receivers, shots = traces.shape
    points = green_rec.shape[3]
    freqs = freq_index.shape[0]
    half = receivers // CORES
    chunks = len(chunks_of(half))
    folds = shots // SUBLANES
    records = jnp.transpose(traces, (0, 2, 1)).reshape(samples, folds, SUBLANES, receivers)
    green = green_rec.reshape(2 * receivers, points)
    sources = green_src.reshape(2 * shots, points)
    block = 2 * shots
    groups = 2 * folds
    bf16, f32 = jnp.bfloat16, jnp.float32
    dma = pltpu.SemaphoreType.DMA
    regular = pltpu.SemaphoreType.REGULAR
    outside = pl.BlockSpec(memory_space=pltpu.HBM)
    piece = (CORES * groups, SUBLANES, half)
    direct = (ROWS * CORES * groups, SUBLANES, chunks_of(half)[DIRECT][1])
    image = pl.pallas_call(
        imaging_kernel,
        out_shape=jax.ShapeDtypeStruct((1, LANES), f32),
        in_specs=[outside] * 5,
        out_specs=pl.BlockSpec(memory_space=pltpu.VMEM),
        scratch_shapes=[
            pltpu.SMEM(freq_index.shape, jnp.int32),
            pltpu.VMEM((samples, folds, SUBLANES, half), bf16),
            pltpu.VMEM((samples, folds, SUBLANES, half), bf16),
            pltpu.VMEM((samples, folds, SUBLANES, half), bf16),
            pltpu.VMEM((2 * freqs * SUBLANES, CORES * samples * SUBLANES), bf16),
            pltpu.VMEM((LEGS,) + piece, bf16),
            pltpu.VMEM((LEGS,) + piece, f32),
            pltpu.VMEM((LEGS - 1,) + piece, bf16),
            pltpu.VMEM(piece, bf16),
            pltpu.VMEM(piece, bf16),
            pltpu.VMEM(piece, bf16),
            pltpu.VMEM(piece, bf16),
            pltpu.VMEM((groups, SUBLANES, half), bf16),
            pltpu.VMEM((3 * CORES + 1, groups, SUBLANES, half), bf16),
            pltpu.VMEM((LEGS - 1,) + direct, bf16),
            pltpu.VMEM(direct, f32),
            pltpu.VMEM((LEGS - 1,) + direct, bf16),
            pltpu.VMEM(direct, bf16),
            pltpu.VMEM((groups,) + direct[1:], f32),
            pltpu.VMEM((ROWS * CORES - 1, groups) + direct[1:], bf16),
            pltpu.VMEM((2 * receivers, points), bf16),
            pltpu.VMEM((block, points), bf16),
            pltpu.VMEM(block_map.shape, jnp.int32),
            pltpu.VMEM((block_map.shape[0], points), f32),
            pltpu.VMEM((block, points), f32),
            pltpu.VMEM((shards, 1, LANES), f32),
            pltpu.VMEM((shards, 1, LANES), f32),
            dma((chunks,)),
            dma((chunks,)),
            dma((3,)),
            dma,
            dma,
            dma((chunks,)),
            dma,
            dma((LEGS - 1, chunks)),
            dma,
            dma((chunks,)),
            dma,
            dma,
            dma,
            dma((chunks,)),
            dma((chunks,)),
            dma,
            dma,
            dma,
            dma,
            dma,
            dma,
            regular((PAIR,)),
            regular,
            regular,
        ],
        compiler_params=pltpu.CompilerParams(
            collective_id=0, has_side_effects=True, vmem_limit_bytes=48 * 1024 * 1024
        ),
    )(
        *(
            pltpu.with_memory_space_constraint(array, pltpu.HBM)
            for array in (records, freq_index, block_map, green, sources)
        )
    )
    return image[0, : points // shards]


def moves_less(traces, freq_index, block_map, green_rec):
    shards = lax.axis_size("freq")
    samples, receivers, shots = traces.shape
    freqs = freq_index.shape[0]
    return (
        2 * freqs <= samples
        and freqs == shards
        and shards == 2 * PAIR * ROWS * CORES
        and shots % SUBLANES == 0
        and receivers % (CORES * LANES) == 0
        and receivers >= CORES * 5 * LANES
        and LANES % (receivers // block_map.shape[0]) == 0
        and green_rec.shape[3] % LANES == 0
        and green_rec.shape[3] // shards <= LANES
    )


def chosen_body(traces, freq_index, block_map, green_rec, green_src):
    fused = moves_less(traces, freq_index, block_map, green_rec)
    return (fused_body if fused else body)(traces, freq_index, block_map, green_rec, green_src)


def solution(mesh):
    in_specs = (
        P("freq", None, "groups"),
        P(),
        P(),
        P("freq", None, None, "groups"),
        P("freq", None, None, "groups"),
    )
    out_specs = P(("groups", "freq"))
    return jax.shard_map(chosen_body, mesh=mesh, in_specs=in_specs, out_specs=out_specs, check_vma=False)
```

```python
import functools
import math

import jax
import jax.numpy as jnp
from jax import lax
from jax.experimental import pallas as pl
from jax.experimental.pallas import tpu as pltpu
from jax.sharding import PartitionSpec as P


def dft_table(freq_index, length):
    sample_index = jnp.arange(length, dtype=jnp.int32)
    phases = freq_index[:, None] * sample_index[None, :] % length
    angles = phases.astype(jnp.float32) * jnp.float32(2.0 * math.pi / length)
    stacked = jnp.stack((jnp.cos(angles), -jnp.sin(angles)), axis=1)
    return stacked.reshape(freq_index.shape[0] * 2, length).astype(jnp.bfloat16)


def expand_map(block_map, receivers, points):
    row_span = receivers // block_map.shape[0]
    col_span = points // block_map.shape[1]
    return jnp.repeat(jnp.repeat(block_map, row_span, axis=0), col_span, axis=1).astype(
        jnp.bfloat16
    )


def transform(cos_table, records, length):
    spectrum = jnp.dot(cos_table, records.reshape(length, -1), preferred_element_type=jnp.float32)
    return (spectrum * (1.0 / math.sqrt(length))).astype(jnp.bfloat16)


def back_project(spectra, masked):
    swapped = jnp.stack((spectra[:, 1], -spectra[:, 0]), axis=1)
    blocks = jnp.stack((spectra, swapped), axis=1)
    return jnp.einsum("fcrx,focrs->fosx", masked, blocks, preferred_element_type=jnp.float32)


def body(traces, freq_index, block_map, green_rec, green_src):
    shards = lax.axis_size("freq")
    length = traces.shape[0] * shards
    receivers = traces.shape[1]
    shots = traces.shape[2]
    freqs = freq_index.shape[0]
    cos_table = dft_table(freq_index, length)
    masked = green_rec * expand_map(block_map, receivers, green_rec.shape[3])[None, None]
    regrouped = lax.all_to_all(traces, "freq", split_axis=2, concat_axis=0, tiled=True)
    spectrum = transform(cos_table, regrouped, length).reshape(freqs, 2, receivers, shots // shards)
    gathered = lax.all_to_all(spectrum, "freq", split_axis=0, concat_axis=3, tiled=True)
    back_field = back_project(gathered, masked)
    partial_image = jnp.sum(green_src.astype(jnp.float32) * back_field, axis=(0, 1, 2))
    return lax.psum_scatter(partial_image, "freq", scatter_dimension=0, tiled=True)


CORES = 2
ROWS = 2
PAIR = 2
LANES = 128
SUBLANES = 8
LEGS = 4
DIRECT = 1
WIDE = 2 * LANES
PIECE = LANES
AHEAD = 2
MIXED = True
MASK = 3.6
LATE = -0.1


def groups_of(half):
    sizes = [LANES, LANES]
    while sum(sizes) < half:
        sizes.append(min(WIDE, half - sum(sizes)))
    return tuple((sum(sizes[:k]), size) for k, size in enumerate(sizes))


def pieces_of(group):
    start, size = group
    return tuple((lane, min(PIECE, start + size - lane)) for lane in range(start, start + size, PIECE))


def chunks_of(half):
    return tuple(piece for group in groups_of(half) for piece in pieces_of(group))


def seat(col, row, core):
    return (col * ROWS + row) * CORES + core


def remote(src, dst, send_sem, recv_sem, target):
    return pltpu.make_async_remote_copy(
        src_ref=src,
        dst_ref=dst,
        send_sem=send_sem,
        recv_sem=recv_sem,
        device_id={"freq": target},
        device_id_type=pl.DeviceIdType.MESH,
    )


def imaging_kernel(*refs):
    half = refs[9].shape[0] * LANES
    chunks = len(chunks_of(half))
    packs = len(groups_of(half))
    dma = pltpu.SemaphoreType.DMA
    pl.run_scoped(
        functools.partial(imaging, *refs),
        dma((packs,)),
        dma((packs,)),
        dma((3,)),
        dma,
        dma,
        dma((packs,)),
        dma,
        dma((LEGS - 1, chunks)),
        dma,
        dma((chunks,)),
        dma,
        dma,
        dma,
        dma((chunks,)),
        dma((chunks,)),
        dma,
        dma,
        dma,
        dma,
        dma,
        dma,
    )


def imaging(
    x_ref,
    fi_hbm,
    map_ref,
    green_ref,
    src_ref,
    out_ref,
    fi_ref,
    x_out,
    x_near,
    x_far,
    table,
    y_send,
    y_keep,
    y_recv,
    relay_send,
    relay_recv,
    cross_send,
    close_send,
    own_send,
    fin,
    d_send,
    d_keep,
    d_recv,
    d_sum,
    d_own,
    d_fin,
    green_v,
    src_v,
    map_v,
    mask_v,
    acc,
    flat,
    i_recv,
    line_sem,
    pair_sem,
    row_sem,
    out_sem,
    near_sem,
    load_sem,
    green_sem,
    far_send,
    far_recv,
    ys_sem,
    yr_sem,
    rs_sem,
    rr_sem,
    cs_sem,
    ns_sem,
    os_sem,
    fin_sem,
    last_sem,
    ds_sem,
    dr_sem,
    dp_sem,
    df_sem,
    is_sem,
    ir_sem,
):
    shards = i_recv.shape[0]
    cols = shards // (ROWS * CORES)
    blocks, folds, samples = x_far.shape[:3]
    half = blocks * LANES
    length = samples * shards
    steps = chunks_of(half)
    chunks = len(steps)
    packs = groups_of(half)
    members = [[k for k in range(chunks) if p <= steps[k][0] < p + n] for p, n in packs]
    folded = [g for g in range(len(packs)) if g != DIRECT]
    order = folded[:AHEAD] + [DIRECT] + folded[AHEAD:]
    freqs = fi_ref.shape[0]
    points = acc.shape[1]
    block = acc.shape[0]
    groups = 2 * folds
    depth = samples * SUBLANES
    bf16, f32 = jnp.bfloat16, jnp.float32

    me = lax.axis_index("freq")
    core = lax.rem(me, CORES)
    row = lax.rem(me // CORES, ROWS)
    col = me // (CORES * ROWS)
    near_col = col + 1 - 2 * lax.rem(col, PAIR)
    cross_col = lax.rem(col + PAIR, cols)
    far_col = lax.rem(near_col + PAIR, cols)
    leg_cols = (far_col, cross_col, near_col, col)
    mate = seat(col, row, 1 - core)
    across = seat(col, 1 - row, core)

    barrier = pltpu.get_barrier_semaphore()

    def tell(sem, target):
        pl.semaphore_signal(
            sem, inc=1, device_id={"freq": target}, device_id_type=pl.DeviceIdType.MESH
        )

    def tell_line(sem):
        @pl.when(col > 0)
        def _():
            tell(sem, seat(col - 1, row, core))

        @pl.when(col < cols - 1)
        def _():
            tell(sem, seat(col + 1, row, core))

    beside = jnp.minimum(col, 1) + jnp.minimum(cols - 1 - col, 1)

    def at(k):
        return pl.ds(*steps[k])

    def lanes(core_at, k):
        return pl.ds(pl.multiple_of(core_at * half + steps[k][0], LANES), steps[k][1])

    def blocks_of(k):
        return pl.ds(packs[k][0] // LANES, packs[k][1] // LANES)

    def x_load(core_at, ref, sem, k):
        start, size = packs[k]
        for lane in range(start, start + size, LANES):
            origin = pl.ds(pl.multiple_of(core_at * half + lane, LANES), LANES)
            for fold in range(folds):
                pltpu.make_async_copy(
                    x_ref.at[:, fold, :, origin], ref.at[lane // LANES, fold], sem.at[k]
                ).start()

    def x_wait(ref, sem, k):
        whole = ref.at[blocks_of(k)]
        pltpu.make_async_copy(whole, whole, sem.at[k]).wait()

    def far_copy(k):
        return remote(
            x_out.at[blocks_of(k)], x_far.at[blocks_of(k)], far_send, far_recv.at[k], mate
        )

    def green_load(k, side, part):
        core_at = core if side == 0 else 1 - core
        start, size = packs[k]
        place = CORES * 2 * start + (2 * side + part) * size
        origin = pl.multiple_of(part * CORES * half + core_at * half + start, LANES)
        return pltpu.make_async_copy(
            green_ref.at[pl.ds(origin, size), :], green_v.at[pl.ds(place, size), :], green_sem
        )

    fi_load = pltpu.make_async_copy(fi_hbm, fi_ref, load_sem.at[0])
    map_load = pltpu.make_async_copy(map_ref, map_v, load_sem.at[1])
    src_load = pltpu.make_async_copy(src_ref, src_v, load_sem.at[2])
    tell(barrier, mate)
    tell(barrier, across)
    x_load(1 - core, x_out, out_sem, order[0])
    fi_load.start()
    tell_line(barrier)
    for k, later in zip(order, order[1:]):
        x_load(1 - core, x_out, out_sem, later)
        x_load(core, x_near, near_sem, k)
    x_load(core, x_near, near_sem, order[-1])

    table_rows = 2 * freqs
    span = CORES * samples
    line = lax.broadcasted_iota(jnp.int32, (table_rows, span), 0)
    column = lax.broadcasted_iota(jnp.int32, (table_rows, span), 1)
    wide = span * SUBLANES
    spread = lax.broadcasted_iota(jnp.int32, (span, wide), 1) // SUBLANES == lax.broadcasted_iota(
        jnp.int32, (span, wide), 0
    )
    pl.semaphore_wait(barrier, 2 + beside)
    x_wait(x_out, out_sem, order[0])
    far_copy(order[0]).start()
    fi_load.wait()
    bins = jnp.zeros((table_rows, span), jnp.int32)
    for side in range(ROWS):
        for leg in range(LEGS):
            for k in range(CORES):
                to_row = 1 - row if side == 0 else row
                place = (side * LEGS + leg) * CORES + k
                bins = jnp.where(line // 2 == place, fi_ref[seat(leg_cols[leg], to_row, k)], bins)
    time = jnp.where(column < samples, me * samples + column, (mate - 1) * samples + column)
    angles = lax.rem(bins * time, length).astype(f32) * f32(2.0 * math.pi / length)
    small = jnp.where(line % 2 == 0, jnp.cos(angles), -jnp.sin(angles)).astype(bf16)
    stretched = jnp.dot(small, jnp.where(spread, 1.0, 0.0).astype(bf16), preferred_element_type=f32)
    same_shot = lax.broadcasted_iota(jnp.int32, (SUBLANES, wide), 1) % SUBLANES == (
        lax.broadcasted_iota(jnp.int32, (SUBLANES, wide), 0)
    )
    for r in range(table_rows):
        spread_row = jnp.broadcast_to(stretched[r : r + 1, :], (SUBLANES, wide))
        table[r * SUBLANES : (r + 1) * SUBLANES, :] = jnp.where(same_shot, spread_row, 0.0).astype(
            bf16
        )

    tell_line(line_sem.at[0])

    def hand_over(k):
        x_wait(x_out, out_sem, k)
        far_copy(k).start()

    hand_over(order[1])
    map_load.start()
    src_load.start()

    def start_green(k):
        for side in range(CORES):
            for part in range(2):
                green_load(k, side, part).start()

    rows = LEGS * CORES * 2 * SUBLANES

    def partial(side, fold, k):
        start, size = packs[k]
        total = None
        for part, ref in enumerate((x_near, x_far)):
            seen = jnp.concatenate(
                [ref[start // LANES + n, fold].reshape(depth, LANES) for n in range(size // LANES)],
                axis=1,
            )
            weights = table[side * rows : (side + 1) * rows, part * depth : (part + 1) * depth]
            term = jnp.dot(weights, seen, preferred_element_type=f32)
            total = term if total is None else total + term
        return total

    def fill(ref, side, k):
        for fold in range(folds):
            total = partial(side, fold, k)
            for leg in range(LEGS):
                for line_at in range(2 * CORES):
                    first = (leg * 2 * CORES + line_at) * SUBLANES
                    ref[leg, line_at * folds + fold, :, pl.ds(*packs[k])] = total[
                        first : first + SUBLANES
                    ].astype(ref.dtype)

    def y_copy(leg, k):
        return remote(
            y_send.at[leg, :, :, at(k)],
            y_recv.at[leg, :, :, at(k)],
            ys_sem,
            yr_sem.at[leg, k],
            across,
        )

    def pick(core_at):
        return pl.ds(core_at * groups, groups)

    def deliver(src_ref_at, kind, k, sem, arrived, to_col, to_row):
        for side in range(CORES):
            to_core = core if side == 0 else 1 - core
            remote(
                src_ref_at(to_core),
                fin.at[kind * CORES + side, :, :, at(k)],
                sem,
                arrived,
                seat(to_col, to_row, to_core),
            ).start()

    def last_copies(k):
        deliver(
            lambda c: y_send.at[LEGS - 1, pick(c), :, at(k)], 0, k, ys_sem, last_sem.at[k], col, 1 - row
        )

    def own_copy(k):
        return remote(
            own_send.at[:, :, at(k)], fin.at[3 * CORES, :, :, at(k)], os_sem, fin_sem.at[k], mate
        )

    def send_partial(k):
        x_wait(x_near, near_sem, k)
        far_copy(k).wait_recv()
        fill(y_send, 0, k)

    def keep_partial(k):
        fill(y_keep, 1, k)
        lane = pl.ds(*packs[k])
        own_send[:, :, lane] = y_keep[LEGS - 1, pick(1 - core), :, lane].astype(bf16)
        for m in members[k]:
            own_copy(m).start()

    def relay_copy(k):
        return remote(
            relay_send.at[:, :, at(k)],
            relay_recv.at[:, :, at(k)],
            rs_sem,
            rr_sem.at[k],
            seat(near_col, row, core),
        )

    def joined(leg, k):
        y_copy(leg, k).wait_recv()
        return y_keep[leg, :, :, at(k)] + y_recv[leg, :, :, at(k)].astype(f32)

    def pass_on(k):
        relay_send[:, :, at(k)] = joined(0, k).astype(bf16)
        relay_copy(k).start()

    def cross(k):
        total = joined(1, k)
        relay_copy(k).wait_recv()
        cross_send[:, :, at(k)] = (total + relay_recv[:, :, at(k)].astype(f32)).astype(bf16)
        deliver(lambda c: cross_send.at[pick(c), :, at(k)], 2, k, cs_sem, fin_sem.at[k], cross_col, row)

    def close(k):
        close_send[:, :, at(k)] = joined(2, k).astype(bf16)
        deliver(lambda c: close_send.at[pick(c), :, at(k)], 1, k, ns_sem, fin_sem.at[k], near_col, row)

    def direct_copy(leg):
        return remote(
            d_send.at[leg], d_recv.at[leg], ds_sem, dr_sem, seat(leg_cols[leg], row, core)
        )

    def send_direct():
        x_wait(x_near, near_sem, DIRECT)
        far_copy(DIRECT).wait_recv()
        for side in range(ROWS):
            for fold in range(folds):
                total = partial(side, fold, DIRECT)
                for leg in range(LEGS):
                    for line_at in range(2 * CORES):
                        first = (leg * 2 * CORES + line_at) * SUBLANES
                        place = (side * 2 * CORES + line_at) * folds + fold
                        value = total[first : first + SUBLANES]
                        if leg < LEGS - 1:
                            d_send[leg, place] = value.astype(bf16)
                        else:
                            d_keep[place] = value
        for leg in range(LEGS - 1):
            direct_copy(leg).start()

    def join_direct():
        pltpu.make_async_copy(d_recv, d_recv, dr_sem).wait()
        total = d_keep[...]
        for leg in range(LEGS - 1):
            total = total + d_recv[leg].astype(f32)
        d_keep[...] = total
        d_sum[...] = total.astype(bf16)
        d_own[...] = d_keep[pl.ds((CORES + core) * groups, groups)]
        for slot, side, to_core, target in (
            (1, 0, core, across),
            (2, 0, 1 - core, seat(col, 1 - row, 1 - core)),
            (0, 1, 1 - core, mate),
        ):
            remote(
                d_sum.at[pl.ds((side * CORES + to_core) * groups, groups)],
                d_fin.at[slot],
                dp_sem,
                df_sem,
                target,
            ).start()

    tiles = map_v.shape[1]

    def make_mask():
        map_load.wait()
        pltpu.make_async_copy(green_v, green_v, green_sem).wait()
        in_tile = lax.broadcasted_iota(jnp.int32, (tiles, points), 1) // (
            points // tiles
        ) == lax.broadcasted_iota(jnp.int32, (tiles, points), 0)
        mask_v[...] = jnp.dot(
            map_v[...].astype(f32).astype(bf16),
            jnp.where(in_tile, 1.0, 0.0).astype(bf16),
            preferred_element_type=f32,
        )
        acc[...] = jnp.zeros_like(acc)

    deep = CORES * half // map_v.shape[0]

    def mask_chunk(k):
        start, size = packs[k]
        for side in range(CORES):
            core_at = core if side == 0 else 1 - core
            for i in range(size // deep):
                seen = mask_v[pl.ds((core_at * half + start) // deep + i, 1), :]
                seen = jnp.broadcast_to(seen, (deep, points)).astype(bf16)
                for part in range(2):
                    place = CORES * 2 * start + (2 * side + part) * size + i * deep
                    green_v[place : place + deep, :] = green_v[place : place + deep, :] * seen

    def use(k, totals):
        start, size = packs[k]
        parts = []
        for total in totals:
            spectrum = total.reshape(block, size) * f32(1.0 / math.sqrt(length))
            turned = jnp.concatenate((spectrum[block // 2 :], -spectrum[: block // 2]), axis=0)
            parts += [spectrum.astype(bf16), turned.astype(bf16)]
        acc[...] += jnp.dot(
            jnp.concatenate(parts, axis=1),
            green_v[CORES * 2 * start : CORES * 2 * (start + size), :],
            preferred_element_type=f32,
        )

    def consume(g):
        lane = pl.ds(*packs[g])
        for k in members[g]:
            wait_fin(k)
        own = y_keep[LEGS - 1, pick(core), :, lane]
        sums = []
        for side in range(CORES):
            total = own if side == 0 else fin[3 * CORES, :, :, lane].astype(f32)
            sums.append(
                total
                + fin[CORES + side, :, :, lane].astype(f32)
                + fin[2 * CORES + side, :, :, lane].astype(f32)
            )
        for k in members[g]:
            wait_last(k)
        use(g, [sums[side] + fin[side, :, :, lane].astype(f32) for side in range(CORES)])

    def consume_direct():
        pltpu.make_async_copy(d_fin, d_fin, df_sem).wait()
        use(
            DIRECT,
            [
                d_own[...] + d_fin[1].astype(f32),
                d_fin[0].astype(f32) + d_fin[2].astype(f32),
            ],
        )

    def wait_fin(k):
        five = fin.at[pl.ds(CORES, 2 * CORES + 1), :, :, at(k)]
        pltpu.make_async_copy(five, five, fin_sem.at[k]).wait()

    def wait_last(k):
        two = fin.at[pl.ds(0, CORES), :, :, at(k)]
        pltpu.make_async_copy(two, two, last_sem.at[k]).wait()

    wire = 0.7 / (2 * LANES)
    hop = 2.6
    clock = 0.0
    arrival = {}

    def expect(leg, k):
        nonlocal clock
        clock += steps[k][1] * wire
        arrival[leg, k] = clock

    def start_y(leg, ks):
        for k in ks:
            expect(leg, k)
            if leg < LEGS - 1:
                y_copy(leg, k).start()
            else:
                last_copies(k)

    def flat_of(groups_at):
        return [k for g in groups_at for k in members[g]]

    kept = 0
    for place, g in enumerate(order):
        if place + 2 < len(order):
            hand_over(order[place + 2])
        if g == DIRECT:
            pl.semaphore_wait(line_sem.at[1], beside)
            tell(pair_sem, mate)
            send_direct()
            continue
        send_partial(g)
        start_y(0, members[g])
        if g == folded[0]:
            start_y(1, members[g])
            clock = max(clock, 0.85)
            pl.semaphore_wait(line_sem.at[0], beside)
            tell_line(line_sem.at[1])
        elif place > 1:
            keep_partial(folded[kept])
            kept += 1
    for g in range(len(packs)):
        start_green(g)
    turns = [(1, k) for k in flat_of(folded[1:])]
    others = [(2, k) for k in flat_of(folded)]
    if MIXED:
        turns = [t for pair in zip(turns, others) for t in pair] + others[len(turns) :]
    else:
        turns += others
    for leg, k in turns:
        start_y(leg, [k])
    tail = flat_of(folded[-1:])
    pl.semaphore_wait(pair_sem, 1)
    tell(row_sem, across)
    start_y(LEGS - 1, flat_of(folded[:-1]))

    def send_last():
        join_direct()
        for k in tail:
            last_copies(k)

    for k in tail:
        expect(LEGS - 1, k)
    events = [(6.2, 7, send_last), (MASK, 5, make_mask)]
    for place, g in enumerate(folded[kept:]):
        events.append((max(arrival[0, members[g][0]] - 0.6, 0.4), 8, lambda g=g: keep_partial(g)))
    mid = 0.0
    for g in folded:
        done = 0.0
        for k in members[g]:
            span = steps[k][1] * wire
            events.append((arrival[0, k], 0, lambda k=k: pass_on(k)))
            merged = max(arrival[1, k], arrival[0, k] + span + hop)
            events.append((merged, 1, lambda k=k: cross(k)))
            mid = max(mid, merged) + 2 * span
            events.append((arrival[2, k], 2, lambda k=k: close(k)))
            done = max(mid + hop + 0.5, arrival[2, k] + span + hop, arrival[LEGS - 1, k], done)
        events.append((done, 4, lambda g=g: consume(g)))
    events.append((done + LATE, 9, consume_direct))
    for g in range(len(packs)):
        events.append((MASK + 0.4 + 0.6 * g, 6, lambda g=g: mask_chunk(g)))
    for _, _, run in sorted(events, key=lambda e: e[:2]):
        run()

    src_load.wait()
    product = src_v[...].astype(f32) * acc[...]
    stacked = product[0:SUBLANES]
    for first in range(SUBLANES, block, SUBLANES):
        stacked = stacked + product[first : first + SUBLANES]
    flat[...] = jnp.sum(stacked, axis=0, keepdims=True)
    each = points // shards

    def window(d):
        first = jnp.minimum(d * each // LANES, points // LANES - 2)
        return pl.ds(pl.multiple_of(first * LANES, LANES), 2 * LANES)

    peers = []
    for leg_col in leg_cols:
        for to_row in (1 - row, row):
            for to_core in (1 - core, core):
                peers.append(seat(leg_col, to_row, to_core))

    def i_copy(slot):
        to = peers[slot]
        return remote(flat.at[:, window(to)], i_recv.at[slot], is_sem, ir_sem, to)

    pl.semaphore_wait(row_sem, 1)
    for slot in range(shards - 1):
        i_copy(slot).start()
    total = flat[:, window(me)]
    others = i_recv.at[pl.ds(0, shards - 1)]
    rest = pl.ds(0, half - packs[DIRECT][1])
    for sent, sem in (
        (x_out, far_send),
        (y_send.at[:, :, :, rest], ys_sem),
        (relay_send.at[:, :, rest], rs_sem),
        (cross_send.at[:, :, rest], cs_sem),
        (close_send.at[:, :, rest], ns_sem),
        (own_send.at[:, :, rest], os_sem),
        (d_send, ds_sem),
        (d_fin, dp_sem),
    ):
        pltpu.make_async_copy(sent, sent, sem).wait()
    pltpu.make_async_copy(others, others, ir_sem).wait()
    for slot in range(shards - 1):
        total = total + i_recv[slot]
    first = jnp.minimum(me * each // LANES, points // LANES - 2) * LANES
    total = jnp.broadcast_to(total, (SUBLANES, 2 * LANES))
    shift = lax.rem(2 * LANES - (me * each - first), 2 * LANES)
    out_ref[...] = pltpu.roll(total, shift, 1)[0:1, :LANES]
    pltpu.make_async_copy(others, others, is_sem).wait()


def fused_body(traces, freq_index, block_map, green_rec, green_src):
    shards = lax.axis_size("freq")
    samples, receivers, shots = traces.shape
    points = green_rec.shape[3]
    freqs = freq_index.shape[0]
    half = receivers // CORES
    chunks = len(chunks_of(half))
    folds = shots // SUBLANES
    records = jnp.transpose(traces, (0, 2, 1)).reshape(samples, folds, SUBLANES, receivers)
    green = green_rec.reshape(2 * receivers, points)
    sources = green_src.reshape(2 * shots, points)
    block = 2 * shots
    groups = 2 * folds
    bf16, f32 = jnp.bfloat16, jnp.float32
    regular = pltpu.SemaphoreType.REGULAR
    outside = pl.BlockSpec(memory_space=pltpu.HBM)
    piece = (CORES * groups, SUBLANES, half)
    direct = (ROWS * CORES * groups, SUBLANES, groups_of(half)[DIRECT][1])
    image = pl.pallas_call(
        imaging_kernel,
        out_shape=jax.ShapeDtypeStruct((1, LANES), f32),
        in_specs=[outside] * 5,
        out_specs=pl.BlockSpec(memory_space=pltpu.VMEM),
        scratch_shapes=[
            pltpu.SMEM(freq_index.shape, jnp.int32),
            pltpu.VMEM((half // LANES, folds, samples, SUBLANES, LANES), bf16),
            pltpu.VMEM((half // LANES, folds, samples, SUBLANES, LANES), bf16),
            pltpu.VMEM((half // LANES, folds, samples, SUBLANES, LANES), bf16),
            pltpu.VMEM((2 * freqs * SUBLANES, CORES * samples * SUBLANES), bf16),
            pltpu.VMEM((LEGS,) + piece, bf16),
            pltpu.VMEM((LEGS,) + piece, f32),
            pltpu.VMEM((LEGS - 1,) + piece, bf16),
            pltpu.VMEM(piece, bf16),
            pltpu.VMEM(piece, bf16),
            pltpu.VMEM(piece, bf16),
            pltpu.VMEM(piece, bf16),
            pltpu.VMEM((groups, SUBLANES, half), bf16),
            pltpu.VMEM((3 * CORES + 1, groups, SUBLANES, half), bf16),
            pltpu.VMEM((LEGS - 1,) + direct, bf16),
            pltpu.VMEM(direct, f32),
            pltpu.VMEM((LEGS - 1,) + direct, bf16),
            pltpu.VMEM(direct, bf16),
            pltpu.VMEM((groups,) + direct[1:], f32),
            pltpu.VMEM((ROWS * CORES - 1, groups) + direct[1:], bf16),
            pltpu.VMEM((2 * receivers, points), bf16),
            pltpu.VMEM((block, points), bf16),
            pltpu.VMEM(block_map.shape, jnp.int32),
            pltpu.VMEM((block_map.shape[0], points), f32),
            pltpu.VMEM((block, points), f32),
            pltpu.VMEM((1, points), f32),
            pltpu.VMEM((shards, 1, 2 * LANES), f32),
            regular((PAIR,)),
            regular,
            regular,
        ],
        compiler_params=pltpu.CompilerParams(
            collective_id=0, has_side_effects=True, vmem_limit_bytes=48 * 1024 * 1024
        ),
    )(
        *(
            pltpu.with_memory_space_constraint(array, pltpu.HBM)
            for array in (records, freq_index, block_map, green, sources)
        )
    )
    return image[0, : points // shards]


def moves_less(traces, freq_index, block_map, green_rec):
    shards = lax.axis_size("freq")
    samples, receivers, shots = traces.shape
    freqs = freq_index.shape[0]
    return (
        2 * freqs <= samples
        and freqs == shards
        and shards == 2 * PAIR * ROWS * CORES
        and shots % SUBLANES == 0
        and receivers % (CORES * LANES) == 0
        and receivers >= CORES * 5 * LANES
        and LANES % (receivers // block_map.shape[0]) == 0
        and green_rec.shape[3] % LANES == 0
        and green_rec.shape[3] >= 2 * LANES
        and green_rec.shape[3] // shards <= LANES
    )


def chosen_body(traces, freq_index, block_map, green_rec, green_src):
    fused = moves_less(traces, freq_index, block_map, green_rec)
    return (fused_body if fused else body)(traces, freq_index, block_map, green_rec, green_src)


def solution(mesh):
    in_specs = (
        P("freq", None, "groups"),
        P(),
        P(),
        P("freq", None, None, "groups"),
        P("freq", None, None, "groups"),
    )
    out_specs = P(("groups", "freq"))
    return jax.shard_map(chosen_body, mesh=mesh, in_specs=in_specs, out_specs=out_specs, check_vma=False)
```

```python
import functools
import math

import jax
import jax.numpy as jnp
from jax import lax
from jax.experimental import pallas as pl
from jax.experimental.pallas import tpu as pltpu
from jax.sharding import PartitionSpec as P


def dft_table(freq_index, length):
    sample_index = jnp.arange(length, dtype=jnp.int32)
    phases = freq_index[:, None] * sample_index[None, :] % length
    angles = phases.astype(jnp.float32) * jnp.float32(2.0 * math.pi / length)
    stacked = jnp.stack((jnp.cos(angles), -jnp.sin(angles)), axis=1)
    return stacked.reshape(freq_index.shape[0] * 2, length).astype(jnp.bfloat16)


def expand_map(block_map, receivers, points):
    row_span = receivers // block_map.shape[0]
    col_span = points // block_map.shape[1]
    return jnp.repeat(jnp.repeat(block_map, row_span, axis=0), col_span, axis=1).astype(
        jnp.bfloat16
    )


def transform(cos_table, records, length):
    spectrum = jnp.dot(cos_table, records.reshape(length, -1), preferred_element_type=jnp.float32)
    return (spectrum * (1.0 / math.sqrt(length))).astype(jnp.bfloat16)


def back_project(spectra, masked):
    swapped = jnp.stack((spectra[:, 1], -spectra[:, 0]), axis=1)
    blocks = jnp.stack((spectra, swapped), axis=1)
    return jnp.einsum("fcrx,focrs->fosx", masked, blocks, preferred_element_type=jnp.float32)


def body(traces, freq_index, block_map, green_rec, green_src):
    shards = lax.axis_size("freq")
    length = traces.shape[0] * shards
    receivers = traces.shape[1]
    shots = traces.shape[2]
    freqs = freq_index.shape[0]
    cos_table = dft_table(freq_index, length)
    masked = green_rec * expand_map(block_map, receivers, green_rec.shape[3])[None, None]
    regrouped = lax.all_to_all(traces, "freq", split_axis=2, concat_axis=0, tiled=True)
    spectrum = transform(cos_table, regrouped, length).reshape(freqs, 2, receivers, shots // shards)
    gathered = lax.all_to_all(spectrum, "freq", split_axis=0, concat_axis=3, tiled=True)
    back_field = back_project(gathered, masked)
    partial_image = jnp.sum(green_src.astype(jnp.float32) * back_field, axis=(0, 1, 2))
    return lax.psum_scatter(partial_image, "freq", scatter_dimension=0, tiled=True)


CORES = 2
ROWS = 2
PAIR = 2
LANES = 128
SUBLANES = 8
LEGS = 4
DIRECT = 1
WIDE = 2 * LANES
PIECE = LANES
AHEAD = 2
PLAN = ("M0", "P01", "P12", "P23", "C0", "C1", "A0", "P34", "C2", "N4", "C3", "B0", "C4", "K0", "K1")
MIXED = True
MASK = 3.6
LATE = -0.1
SPLIT = 1


def groups_of(half):
    sizes = [LANES, LANES]
    while sum(sizes) < half:
        sizes.append(min(WIDE, half - sum(sizes)))
    return tuple((sum(sizes[:k]), size) for k, size in enumerate(sizes))


def pieces_of(group):
    start, size = group
    return tuple((lane, min(PIECE, start + size - lane)) for lane in range(start, start + size, PIECE))


def chunks_of(half):
    return tuple(piece for group in groups_of(half) for piece in pieces_of(group))


def seat(col, row, core):
    return (col * ROWS + row) * CORES + core


def remote(src, dst, send_sem, recv_sem, target):
    return pltpu.make_async_remote_copy(
        src_ref=src,
        dst_ref=dst,
        send_sem=send_sem,
        recv_sem=recv_sem,
        device_id={"freq": target},
        device_id_type=pl.DeviceIdType.MESH,
    )


def imaging_kernel(*refs):
    half = refs[8].shape[0] * LANES
    chunks = len(chunks_of(half))
    packs = len(groups_of(half))
    dma = pltpu.SemaphoreType.DMA
    pl.run_scoped(
        functools.partial(imaging, *refs),
        dma((packs,)),
        dma((packs,)),
        dma((3,)),
        dma,
        dma,
        dma((packs,)),
        dma,
        dma((LEGS - 1, chunks)),
        dma,
        dma((chunks,)),
        dma,
        dma,
        dma,
        dma((chunks,)),
        dma((chunks,)),
        dma,
        dma,
        dma,
        dma,
        dma,
        dma,
    )


def imaging(
    x_ref,
    fi_hbm,
    map_ref,
    green_ref,
    src_ref,
    out_ref,
    fi_ref,
    x_out,
    x_near,
    table,
    p_send,
    p_recv,
    near,
    y_send,
    y_recv,
    relay_send,
    relay_recv,
    cross_send,
    close_send,
    own_send,
    fin,
    d_send,
    d_keep,
    d_recv,
    d_sum,
    d_own,
    d_fin,
    green_v,
    src_v,
    map_v,
    mask_v,
    acc,
    flat,
    i_recv,
    line_sem,
    pair_sem,
    row_sem,
    out_sem,
    near_sem,
    load_sem,
    green_sem,
    far_send,
    far_recv,
    ys_sem,
    yr_sem,
    rs_sem,
    rr_sem,
    cs_sem,
    ns_sem,
    os_sem,
    fin_sem,
    last_sem,
    ds_sem,
    dr_sem,
    dp_sem,
    df_sem,
    is_sem,
    ir_sem,
):
    shards = i_recv.shape[0]
    cols = shards // (ROWS * CORES)
    blocks, folds, samples = x_near.shape[:3]
    half = blocks * LANES
    length = samples * shards
    steps = chunks_of(half)
    chunks = len(steps)
    packs = groups_of(half)
    members = [[k for k in range(chunks) if p <= steps[k][0] < p + n] for p, n in packs]
    folded = [g for g in range(len(packs)) if g != DIRECT]
    order = folded[:AHEAD] + [DIRECT] + folded[AHEAD:]
    freqs = fi_ref.shape[0]
    points = acc.shape[1]
    block = acc.shape[0]
    groups = 2 * folds
    depth = samples * SUBLANES
    bf16, f32 = jnp.bfloat16, jnp.float32

    me = lax.axis_index("freq")
    core = lax.rem(me, CORES)
    row = lax.rem(me // CORES, ROWS)
    col = me // (CORES * ROWS)
    near_col = col + 1 - 2 * lax.rem(col, PAIR)
    cross_col = lax.rem(col + PAIR, cols)
    far_col = lax.rem(near_col + PAIR, cols)
    leg_cols = (far_col, cross_col, near_col, col)
    mate = seat(col, row, 1 - core)
    across = seat(col, 1 - row, core)

    barrier = pltpu.get_barrier_semaphore()

    def tell(sem, target):
        pl.semaphore_signal(
            sem, inc=1, device_id={"freq": target}, device_id_type=pl.DeviceIdType.MESH
        )

    def tell_line(sem):
        @pl.when(col > 0)
        def _():
            tell(sem, seat(col - 1, row, core))

        @pl.when(col < cols - 1)
        def _():
            tell(sem, seat(col + 1, row, core))

    beside = jnp.minimum(col, 1) + jnp.minimum(cols - 1 - col, 1)

    def at(k):
        return pl.ds(*steps[k])

    def lanes(core_at, k):
        return pl.ds(pl.multiple_of(core_at * half + steps[k][0], LANES), steps[k][1])

    def blocks_of(k):
        return pl.ds(packs[k][0] // LANES, packs[k][1] // LANES)

    def x_load(core_at, ref, sem, k):
        start, size = packs[k]
        for lane in range(start, start + size, LANES):
            origin = pl.ds(pl.multiple_of(core_at * half + lane, LANES), LANES)
            for fold in range(folds):
                pltpu.make_async_copy(
                    x_ref.at[:, fold, :, origin], ref.at[lane // LANES, fold], sem.at[k]
                ).start()

    def x_wait(ref, sem, k):
        whole = ref.at[blocks_of(k)]
        pltpu.make_async_copy(whole, whole, sem.at[k]).wait()

    def span_of(g):
        return pl.ds(*packs[g])

    def far_copy(g):
        return remote(
            p_send.at[:, :, :, :, span_of(g)],
            p_recv.at[:, :, :, :, span_of(g)],
            far_send,
            far_recv.at[g],
            mate,
        )

    def green_place(lane, side, part):
        return CORES * 2 * lane + (2 * side + part) * LANES

    def green_load(lane, side, part):
        core_at = core if side == 0 else 1 - core
        origin = pl.multiple_of(part * CORES * half + core_at * half + lane, LANES)
        return pltpu.make_async_copy(
            green_ref.at[pl.ds(origin, LANES), :],
            green_v.at[pl.ds(green_place(lane, side, part), LANES), :],
            green_sem,
        )

    fi_load = pltpu.make_async_copy(fi_hbm, fi_ref, load_sem.at[0])
    map_load = pltpu.make_async_copy(map_ref, map_v, load_sem.at[1])
    src_load = pltpu.make_async_copy(src_ref, src_v, load_sem.at[2])
    tell(barrier, mate)
    tell(barrier, across)
    x_load(1 - core, x_out, out_sem, order[0])
    fi_load.start()
    tell_line(barrier)
    for k, later in zip(order, order[1:]):
        x_load(1 - core, x_out, out_sem, later)
        x_load(core, x_near, near_sem, k)
    x_load(core, x_near, near_sem, order[-1])

    table_rows = 2 * freqs
    line = lax.broadcasted_iota(jnp.int32, (table_rows, samples), 0)
    column = lax.broadcasted_iota(jnp.int32, (table_rows, samples), 1)
    spread = lax.broadcasted_iota(jnp.int32, (samples, depth), 1) // SUBLANES == (
        lax.broadcasted_iota(jnp.int32, (samples, depth), 0)
    )
    fi_load.wait()
    bins = jnp.zeros((table_rows, samples), jnp.int32)
    for side in range(ROWS):
        for leg in range(LEGS):
            for k in range(CORES):
                to_row = 1 - row if side == 0 else row
                place = (side * LEGS + leg) * CORES + k
                bins = jnp.where(line // 2 == place, fi_ref[seat(leg_cols[leg], to_row, k)], bins)
    angles = lax.rem(bins * (me * samples + column), length).astype(f32) * f32(
        2.0 * math.pi / length
    )
    small = jnp.where(line % 2 == 0, jnp.cos(angles), -jnp.sin(angles)).astype(bf16)
    stretched = jnp.dot(small, jnp.where(spread, 1.0, 0.0).astype(bf16), preferred_element_type=f32)
    same_shot = lax.broadcasted_iota(jnp.int32, (SUBLANES, depth), 1) % SUBLANES == (
        lax.broadcasted_iota(jnp.int32, (SUBLANES, depth), 0)
    )
    for r in range(table_rows):
        spread_row = jnp.broadcast_to(stretched[r : r + 1, :], (SUBLANES, depth))
        table[r * SUBLANES : (r + 1) * SUBLANES, :] = jnp.where(same_shot, spread_row, 0.0).astype(
            bf16
        )

    def lanes_of(k):
        return range(packs[k][0], packs[k][0] + packs[k][1], LANES)

    def start_green(k):
        for lane in lanes_of(k):
            for side in range(CORES):
                for part in range(2):
                    green_load(lane, side, part).start()

    def transform(x_at, ref, g):
        start, size = packs[g]
        for fold in range(folds):
            seen = jnp.concatenate(
                [
                    x_at[start // LANES + n, fold].reshape(depth, LANES)
                    for n in range(size // LANES)
                ],
                axis=1,
            )
            total = jnp.dot(table[...], seen, preferred_element_type=f32)
            for side in range(ROWS):
                for leg in range(LEGS):
                    for line_at in range(2 * CORES):
                        first = ((side * LEGS + leg) * 2 * CORES + line_at) * SUBLANES
                        ref[side, leg, line_at * folds + fold, :, span_of(g)] = total[
                            first : first + SUBLANES
                        ].astype(ref.dtype)

    def hand_over(g):
        x_wait(x_out, out_sem, g)
        transform(x_out, p_send, g)

    def keep_near(g):
        x_wait(x_near, near_sem, g)
        transform(x_near, near, g)

    def y_copy(leg, k):
        return remote(
            y_send.at[leg, :, :, at(k)],
            y_recv.at[leg, :, :, at(k)],
            ys_sem,
            yr_sem.at[leg, k],
            across,
        )

    def pick(core_at):
        return pl.ds(core_at * groups, groups)

    def deliver(src_ref_at, kind, k, sem, arrived, to_col, to_row):
        for side in range(CORES):
            to_core = core if side == 0 else 1 - core
            remote(
                src_ref_at(to_core),
                fin.at[kind * CORES + side, :, :, at(k)],
                sem,
                arrived,
                seat(to_col, to_row, to_core),
            ).start()

    def last_copies(k):
        deliver(
            lambda c: y_send.at[LEGS - 1, pick(c), :, at(k)], 0, k, ys_sem, last_sem.at[k], col, 1 - row
        )

    def own_copy(k):
        return remote(
            own_send.at[:, :, at(k)], fin.at[3 * CORES, :, :, at(k)], os_sem, fin_sem.at[k], mate
        )

    def joint(side, leg, lane):
        return near[side, leg, :, :, lane] + p_recv[side, leg, :, :, lane].astype(f32)

    def send_partial(g):
        far_copy(g).wait_recv()
        for leg in range(LEGS):
            y_send[leg, :, :, span_of(g)] = joint(0, leg, span_of(g)).astype(bf16)

    def keep_partial(g):
        lane = span_of(g)
        for leg in range(LEGS):
            near[1, leg, :, :, lane] = joint(1, leg, lane)
        own_send[:, :, lane] = near[1, LEGS - 1, pick(1 - core), :, lane].astype(bf16)
        for m in members[g]:
            own_copy(m).start()

    def relay_copy(k):
        return remote(
            relay_send.at[:, :, at(k)],
            relay_recv.at[:, :, at(k)],
            rs_sem,
            rr_sem.at[k],
            seat(near_col, row, core),
        )

    def joined(leg, k):
        y_copy(leg, k).wait_recv()
        return near[1, leg, :, :, at(k)] + y_recv[leg, :, :, at(k)].astype(f32)

    def pass_on(k):
        relay_send[:, :, at(k)] = joined(0, k).astype(bf16)
        relay_copy(k).start()

    def cross(k):
        total = joined(1, k)
        relay_copy(k).wait_recv()
        cross_send[:, :, at(k)] = (total + relay_recv[:, :, at(k)].astype(f32)).astype(bf16)
        deliver(lambda c: cross_send.at[pick(c), :, at(k)], 2, k, cs_sem, fin_sem.at[k], cross_col, row)

    def close(k):
        close_send[:, :, at(k)] = joined(2, k).astype(bf16)
        deliver(lambda c: close_send.at[pick(c), :, at(k)], 1, k, ns_sem, fin_sem.at[k], near_col, row)

    def direct_copy(leg):
        return remote(
            d_send.at[leg], d_recv.at[leg], ds_sem, dr_sem, seat(leg_cols[leg], row, core)
        )

    def send_direct():
        far_copy(DIRECT).wait_recv()
        for leg in range(LEGS):
            for side in range(ROWS):
                total = joint(side, leg, span_of(DIRECT))
                places = pl.ds(side * CORES * groups, CORES * groups)
                if leg < LEGS - 1:
                    d_send[leg, places] = total.astype(bf16)
                else:
                    d_keep[places] = total
            if 0 < leg < LEGS - 1:
                direct_copy(leg).start()

    def join_direct():
        pltpu.make_async_copy(d_recv, d_recv, dr_sem).wait()
        total = d_keep[...]
        for leg in range(LEGS - 1):
            total = total + d_recv[leg].astype(f32)
        d_keep[...] = total
        d_sum[...] = total.astype(bf16)
        d_own[...] = d_keep[pl.ds((CORES + core) * groups, groups)]
        for slot, side, to_core, target in (
            (1, 0, core, across),
            (2, 0, 1 - core, seat(col, 1 - row, 1 - core)),
            (0, 1, 1 - core, mate),
        ):
            remote(
                d_sum.at[pl.ds((side * CORES + to_core) * groups, groups)],
                d_fin.at[slot],
                dp_sem,
                df_sem,
                target,
            ).start()

    tiles = map_v.shape[1]

    def make_mask():
        map_load.wait()
        pltpu.make_async_copy(green_v, green_v, green_sem).wait()
        in_tile = lax.broadcasted_iota(jnp.int32, (tiles, points), 1) // (
            points // tiles
        ) == lax.broadcasted_iota(jnp.int32, (tiles, points), 0)
        mask_v[...] = jnp.dot(
            map_v[...].astype(f32).astype(bf16),
            jnp.where(in_tile, 1.0, 0.0).astype(bf16),
            preferred_element_type=f32,
        )
        acc[...] = jnp.zeros_like(acc)

    deep = CORES * half // map_v.shape[0]

    def mask_chunk(k):
        for lane in lanes_of(k):
            for side in range(CORES):
                core_at = core if side == 0 else 1 - core
                for i in range(LANES // deep):
                    seen = mask_v[pl.ds((core_at * half + lane) // deep + i, 1), :]
                    seen = jnp.broadcast_to(seen, (deep, points)).astype(bf16)
                    for part in range(2):
                        place = green_place(lane, side, part) + i * deep
                        green_v[place : place + deep, :] = green_v[place : place + deep, :] * seen

    def use(start, size, totals):
        spectra = []
        for total in totals:
            spectrum = total.reshape(block, size) * f32(1.0 / math.sqrt(length))
            turned = jnp.concatenate((spectrum[block // 2 :], -spectrum[: block // 2]), axis=0)
            spectra += [spectrum.astype(bf16), turned.astype(bf16)]
        parts = [
            spectrum[:, lane : lane + LANES] for lane in range(0, size, LANES) for spectrum in spectra
        ]
        acc[...] += jnp.dot(
            jnp.concatenate(parts, axis=1),
            green_v[CORES * 2 * start : CORES * 2 * (start + size), :],
            preferred_element_type=f32,
        )

    def consume(start, size, ks):
        lane = pl.ds(start, size)
        for k in ks:
            wait_fin(k)
        own = near[1, LEGS - 1, pick(core), :, lane]
        sums = []
        for side in range(CORES):
            total = own if side == 0 else fin[3 * CORES, :, :, lane].astype(f32)
            sums.append(
                total
                + fin[CORES + side, :, :, lane].astype(f32)
                + fin[2 * CORES + side, :, :, lane].astype(f32)
            )
        for k in ks:
            wait_last(k)
        use(start, size, [sums[side] + fin[side, :, :, lane].astype(f32) for side in range(CORES)])

    def consume_direct():
        pltpu.make_async_copy(d_fin, d_fin, df_sem).wait()
        use(
            *packs[DIRECT],
            [
                d_own[...] + d_fin[1].astype(f32),
                d_fin[0].astype(f32) + d_fin[2].astype(f32),
            ],
        )

    def wait_fin(k):
        five = fin.at[pl.ds(CORES, 2 * CORES + 1), :, :, at(k)]
        pltpu.make_async_copy(five, five, fin_sem.at[k]).wait()

    def wait_last(k):
        two = fin.at[pl.ds(0, CORES), :, :, at(k)]
        pltpu.make_async_copy(two, two, last_sem.at[k]).wait()

    wire = 0.7 / (2 * LANES)
    hop = 2.6
    clock = 0.0
    arrival = {}

    def expect(leg, k):
        nonlocal clock
        clock += steps[k][1] * wire
        arrival[leg, k] = clock

    def start_y(leg, ks):
        for k in ks:
            expect(leg, k)
            if leg < LEGS - 1:
                y_copy(leg, k).start()
            else:
                last_copies(k)

    def flat_of(groups_at):
        return [k for g in groups_at for k in members[g]]

    def combine(g):
        if g == DIRECT:
            send_direct()
            return
        send_partial(g)
        start_y(0, members[g])
        if g == folded[0]:
            start_y(1, members[g])
            clock_at_least(0.85)

    def clock_at_least(value):
        nonlocal clock
        clock = max(clock, value)

    def advance(token):
        kind, place = token[:2]
        g = order[place] if place < len(order) else None
        if kind == "M":
            hand_over(g)
            if place == 0:
                pl.semaphore_wait(barrier, 2 + beside)
                tell_line(line_sem.at[0])
            far_copy(g).start()
        elif kind == "N":
            keep_near(g)
        elif kind == "P":
            ahead = order[token[2]]
            x_wait(x_near, near_sem, g)
            x_wait(x_out, out_sem, ahead)
            transform(x_out, p_send, ahead)
            transform(x_near, near, g)
            far_copy(ahead).start()
        elif kind == "C":
            combine(g)
        elif kind == "K":
            keep_partial(folded[place])
        elif kind == "A":
            pl.semaphore_wait(line_sem.at[0], beside)
            tell_line(line_sem.at[1])
        else:
            pl.semaphore_wait(line_sem.at[1], beside)
            tell(pair_sem, mate)
            direct_copy(0).start()

    for step in PLAN:
        advance((step[0],) + tuple(int(digit) for digit in step[1:]))
    kept = sum(step[0] == "K" for step in PLAN)
    map_load.start()
    src_load.start()
    for g in range(len(packs)):
        start_green(g)
    turns = [(1, k) for k in flat_of(folded[1:])]
    others = [(2, k) for k in flat_of(folded)]
    if MIXED:
        turns = [t for pair in zip(turns, others) for t in pair] + others[len(turns) :]
    else:
        turns += others
    for leg, k in turns:
        start_y(leg, [k])
    tail = flat_of(folded[-1:])
    pl.semaphore_wait(pair_sem, 1)
    tell(row_sem, across)
    start_y(LEGS - 1, flat_of(folded[:-1]))

    def send_last():
        join_direct()
        for k in tail:
            last_copies(k)

    for k in tail:
        expect(LEGS - 1, k)
    events = [(6.2, 7, send_last), (MASK, 5, make_mask)]
    for place, g in enumerate(folded[kept:]):
        events.append((max(arrival[0, members[g][0]] - 0.6, 0.4), 8, lambda g=g: keep_partial(g)))
    mid = 0.0
    for g in folded:
        done = 0.0
        for k in members[g]:
            span = steps[k][1] * wire
            events.append((arrival[0, k], 0, lambda k=k: pass_on(k)))
            merged = max(arrival[1, k], arrival[0, k] + span + hop)
            events.append((merged, 1, lambda k=k: cross(k)))
            mid = max(mid, merged) + 2 * span
            events.append((arrival[2, k], 2, lambda k=k: close(k)))
            done = max(mid + hop + 0.5, arrival[2, k] + span + hop, arrival[LEGS - 1, k], done)
            if g in folded[len(folded) - SPLIT :]:
                events.append((done, 4, lambda k=k: consume(*steps[k], [k])))
        if g not in folded[len(folded) - SPLIT :]:
            events.append((done, 4, lambda g=g: consume(*packs[g], members[g])))
    events.append((done + LATE, 9, consume_direct))
    for g in range(len(packs)):
        events.append((MASK + 0.4 + 0.6 * g, 6, lambda g=g: mask_chunk(g)))
    for _, _, run in sorted(events, key=lambda e: e[:2]):
        run()

    src_load.wait()
    product = src_v[...].astype(f32) * acc[...]
    stacked = product[0:SUBLANES]
    for first in range(SUBLANES, block, SUBLANES):
        stacked = stacked + product[first : first + SUBLANES]
    flat[...] = jnp.sum(stacked, axis=0, keepdims=True)
    each = points // shards

    def window(d):
        first = jnp.minimum(d * each // LANES, points // LANES - 2)
        return pl.ds(pl.multiple_of(first * LANES, LANES), 2 * LANES)

    peers = []
    for leg_col in leg_cols:
        for to_row in (1 - row, row):
            for to_core in (1 - core, core):
                peers.append(seat(leg_col, to_row, to_core))

    def i_copy(slot):
        to = peers[slot]
        return remote(flat.at[:, window(to)], i_recv.at[slot], is_sem, ir_sem, to)

    pl.semaphore_wait(row_sem, 1)
    for slot in range(shards - 1):
        i_copy(slot).start()
    total = flat[:, window(me)]
    others = i_recv.at[pl.ds(0, shards - 1)]
    rest = pl.ds(0, half - packs[DIRECT][1])
    for sent, sem in (
        (p_send, far_send),
        (y_send.at[:, :, :, rest], ys_sem),
        (relay_send.at[:, :, rest], rs_sem),
        (cross_send.at[:, :, rest], cs_sem),
        (close_send.at[:, :, rest], ns_sem),
        (own_send.at[:, :, rest], os_sem),
        (d_send, ds_sem),
        (d_fin, dp_sem),
    ):
        pltpu.make_async_copy(sent, sent, sem).wait()
    pltpu.make_async_copy(others, others, ir_sem).wait()
    for slot in range(shards - 1):
        total = total + i_recv[slot]
    first = jnp.minimum(me * each // LANES, points // LANES - 2) * LANES
    total = jnp.broadcast_to(total, (SUBLANES, 2 * LANES))
    shift = lax.rem(2 * LANES - (me * each - first), 2 * LANES)
    out_ref[...] = pltpu.roll(total, shift, 1)[0:1, :each]
    pltpu.make_async_copy(others, others, is_sem).wait()


def fused_body(traces, freq_index, block_map, green_rec, green_src):
    shards = lax.axis_size("freq")
    samples, receivers, shots = traces.shape
    points = green_rec.shape[3]
    freqs = freq_index.shape[0]
    half = receivers // CORES
    chunks = len(chunks_of(half))
    folds = shots // SUBLANES
    records = jnp.transpose(traces, (0, 2, 1)).reshape(samples, folds, SUBLANES, receivers)
    green = green_rec.reshape(2 * receivers, points)
    sources = green_src.reshape(2 * shots, points)
    block = 2 * shots
    groups = 2 * folds
    bf16, f32 = jnp.bfloat16, jnp.float32
    regular = pltpu.SemaphoreType.REGULAR
    outside = pl.BlockSpec(memory_space=pltpu.HBM)
    piece = (CORES * groups, SUBLANES, half)
    direct = (ROWS * CORES * groups, SUBLANES, groups_of(half)[DIRECT][1])
    image = pl.pallas_call(
        imaging_kernel,
        out_shape=jax.ShapeDtypeStruct((1, points // shards), f32),
        in_specs=[outside] * 5,
        out_specs=pl.BlockSpec(memory_space=pltpu.VMEM),
        scratch_shapes=[
            pltpu.SMEM(freq_index.shape, jnp.int32),
            pltpu.VMEM((half // LANES, folds, samples, SUBLANES, LANES), bf16),
            pltpu.VMEM((half // LANES, folds, samples, SUBLANES, LANES), bf16),
            pltpu.VMEM((2 * freqs * SUBLANES, samples * SUBLANES), bf16),
            pltpu.VMEM((ROWS, LEGS) + piece, bf16),
            pltpu.VMEM((ROWS, LEGS) + piece, bf16),
            pltpu.VMEM((ROWS, LEGS) + piece, f32),
            pltpu.VMEM((LEGS,) + piece, bf16),
            pltpu.VMEM((LEGS - 1,) + piece, bf16),
            pltpu.VMEM(piece, bf16),
            pltpu.VMEM(piece, bf16),
            pltpu.VMEM(piece, bf16),
            pltpu.VMEM(piece, bf16),
            pltpu.VMEM((groups, SUBLANES, half), bf16),
            pltpu.VMEM((3 * CORES + 1, groups, SUBLANES, half), bf16),
            pltpu.VMEM((LEGS - 1,) + direct, bf16),
            pltpu.VMEM(direct, f32),
            pltpu.VMEM((LEGS - 1,) + direct, bf16),
            pltpu.VMEM(direct, bf16),
            pltpu.VMEM((groups,) + direct[1:], f32),
            pltpu.VMEM((ROWS * CORES - 1, groups) + direct[1:], bf16),
            pltpu.VMEM((2 * receivers, points), bf16),
            pltpu.VMEM((block, points), bf16),
            pltpu.VMEM(block_map.shape, jnp.int32),
            pltpu.VMEM((block_map.shape[0], points), f32),
            pltpu.VMEM((block, points), f32),
            pltpu.VMEM((1, points), f32),
            pltpu.VMEM((shards, 1, 2 * LANES), f32),
            regular((PAIR,)),
            regular,
            regular,
        ],
        compiler_params=pltpu.CompilerParams(
            collective_id=0, has_side_effects=True, vmem_limit_bytes=48 * 1024 * 1024
        ),
    )(
        *(
            pltpu.with_memory_space_constraint(array, pltpu.HBM)
            for array in (records, freq_index, block_map, green, sources)
        )
    )
    return image.reshape(points // shards)


def moves_less(traces, freq_index, block_map, green_rec):
    shards = lax.axis_size("freq")
    samples, receivers, shots = traces.shape
    freqs = freq_index.shape[0]
    return (
        2 * freqs <= samples
        and freqs == shards
        and shards == 2 * PAIR * ROWS * CORES
        and shots % SUBLANES == 0
        and receivers % (CORES * LANES) == 0
        and receivers >= CORES * 5 * LANES
        and LANES % (receivers // block_map.shape[0]) == 0
        and green_rec.shape[3] % LANES == 0
        and green_rec.shape[3] >= 2 * LANES
        and green_rec.shape[3] // shards <= LANES
    )


def chosen_body(traces, freq_index, block_map, green_rec, green_src):
    fused = moves_less(traces, freq_index, block_map, green_rec)
    return (fused_body if fused else body)(traces, freq_index, block_map, green_rec, green_src)


def solution(mesh):
    in_specs = (
        P("freq", None, "groups"),
        P(),
        P(),
        P("freq", None, None, "groups"),
        P("freq", None, None, "groups"),
    )
    out_specs = P(("groups", "freq"))
    return jax.shard_map(chosen_body, mesh=mesh, in_specs=in_specs, out_specs=out_specs, check_vma=False)
```

```python
import functools
import math

import jax
import jax.numpy as jnp
from jax import lax
from jax.experimental import pallas as pl
from jax.experimental.pallas import tpu as pltpu
from jax.sharding import PartitionSpec as P


def dft_table(freq_index, length):
    sample_index = jnp.arange(length, dtype=jnp.int32)
    phases = freq_index[:, None] * sample_index[None, :] % length
    angles = phases.astype(jnp.float32) * jnp.float32(2.0 * math.pi / length)
    stacked = jnp.stack((jnp.cos(angles), -jnp.sin(angles)), axis=1)
    return stacked.reshape(freq_index.shape[0] * 2, length).astype(jnp.bfloat16)


def expand_map(block_map, receivers, points):
    row_span = receivers // block_map.shape[0]
    col_span = points // block_map.shape[1]
    return jnp.repeat(jnp.repeat(block_map, row_span, axis=0), col_span, axis=1).astype(
        jnp.bfloat16
    )


def transform(cos_table, records, length):
    spectrum = jnp.dot(cos_table, records.reshape(length, -1), preferred_element_type=jnp.float32)
    return (spectrum * (1.0 / math.sqrt(length))).astype(jnp.bfloat16)


def back_project(spectra, masked):
    swapped = jnp.stack((spectra[:, 1], -spectra[:, 0]), axis=1)
    blocks = jnp.stack((spectra, swapped), axis=1)
    return jnp.einsum("fcrx,focrs->fosx", masked, blocks, preferred_element_type=jnp.float32)


def body(traces, freq_index, block_map, green_rec, green_src):
    shards = lax.axis_size("freq")
    length = traces.shape[0] * shards
    receivers = traces.shape[1]
    shots = traces.shape[2]
    freqs = freq_index.shape[0]
    cos_table = dft_table(freq_index, length)
    masked = green_rec * expand_map(block_map, receivers, green_rec.shape[3])[None, None]
    regrouped = lax.all_to_all(traces, "freq", split_axis=2, concat_axis=0, tiled=True)
    spectrum = transform(cos_table, regrouped, length).reshape(freqs, 2, receivers, shots // shards)
    gathered = lax.all_to_all(spectrum, "freq", split_axis=0, concat_axis=3, tiled=True)
    back_field = back_project(gathered, masked)
    partial_image = jnp.sum(green_src.astype(jnp.float32) * back_field, axis=(0, 1, 2))
    return lax.psum_scatter(partial_image, "freq", scatter_dimension=0, tiled=True)


CORES = 2
ROWS = 2
PAIR = 2
LANES = 128
SUBLANES = 8
LEGS = 4
DIRECT = 1
WIDE = 2 * LANES
PIECE = LANES
AHEAD = 2
PLAN = ("M0", "P01", "P12", "P23", "C0", "C1", "A0", "P34", "C2", "N4", "C3", "B0", "C4", "K0", "K1")
MIXED = True
MASK = 3.6
LATE = -0.1
SPLIT = 1
LEAD = 0


def groups_of(half):
    sizes = [LANES, LANES]
    while sum(sizes) < half:
        sizes.append(min(WIDE, half - sum(sizes)))
    return tuple((sum(sizes[:k]), size) for k, size in enumerate(sizes))


def pieces_of(group):
    start, size = group
    return tuple((lane, min(PIECE, start + size - lane)) for lane in range(start, start + size, PIECE))


def chunks_of(half):
    return tuple(piece for group in groups_of(half) for piece in pieces_of(group))


def seat(col, row, core):
    return (col * ROWS + row) * CORES + core


def remote(src, dst, send_sem, recv_sem, target):
    return pltpu.make_async_remote_copy(
        src_ref=src,
        dst_ref=dst,
        send_sem=send_sem,
        recv_sem=recv_sem,
        device_id={"freq": target},
        device_id_type=pl.DeviceIdType.MESH,
    )


def imaging_kernel(*refs):
    half = refs[8].shape[0] * LANES
    chunks = len(chunks_of(half))
    packs = len(groups_of(half))
    dma = pltpu.SemaphoreType.DMA
    pl.run_scoped(
        functools.partial(imaging, *refs),
        dma((packs,)),
        dma((packs,)),
        dma((3,)),
        dma,
        dma,
        dma((packs,)),
        dma,
        dma((LEGS - 1, chunks)),
        dma,
        dma((chunks,)),
        dma,
        dma,
        dma,
        dma((chunks,)),
        dma((chunks,)),
        dma,
        dma,
        dma,
        dma,
        dma,
        dma,
    )


def imaging(
    x_ref,
    fi_hbm,
    map_ref,
    green_ref,
    src_ref,
    out_ref,
    fi_ref,
    x_out,
    x_near,
    table,
    p_send,
    p_recv,
    near,
    y_send,
    y_recv,
    relay_send,
    relay_recv,
    cross_send,
    close_send,
    own_send,
    fin,
    d_send,
    d_keep,
    d_recv,
    d_sum,
    d_own,
    d_fin,
    green_v,
    src_v,
    map_v,
    mask_v,
    acc,
    flat,
    i_recv,
    line_sem,
    pair_sem,
    row_sem,
    out_sem,
    near_sem,
    load_sem,
    green_sem,
    far_send,
    far_recv,
    ys_sem,
    yr_sem,
    rs_sem,
    rr_sem,
    cs_sem,
    ns_sem,
    os_sem,
    fin_sem,
    last_sem,
    ds_sem,
    dr_sem,
    dp_sem,
    df_sem,
    is_sem,
    ir_sem,
):
    shards = i_recv.shape[0]
    cols = shards // (ROWS * CORES)
    blocks, folds, samples = x_near.shape[:3]
    half = blocks * LANES
    length = samples * shards
    steps = chunks_of(half)
    chunks = len(steps)
    packs = groups_of(half)
    members = [[k for k in range(chunks) if p <= steps[k][0] < p + n] for p, n in packs]
    folded = [g for g in range(len(packs)) if g != DIRECT]
    order = folded[:AHEAD] + [DIRECT] + folded[AHEAD:]
    freqs = fi_ref.shape[0]
    points = acc.shape[1]
    block = acc.shape[0]
    groups = 2 * folds
    depth = samples * SUBLANES
    bf16, f32 = jnp.bfloat16, jnp.float32

    me = lax.axis_index("freq")
    core = lax.rem(me, CORES)
    row = lax.rem(me // CORES, ROWS)
    col = me // (CORES * ROWS)
    near_col = col + 1 - 2 * lax.rem(col, PAIR)
    cross_col = lax.rem(col + PAIR, cols)
    far_col = lax.rem(near_col + PAIR, cols)
    leg_cols = (far_col, cross_col, near_col, col)
    mate = seat(col, row, 1 - core)
    across = seat(col, 1 - row, core)

    barrier = pltpu.get_barrier_semaphore()

    def tell(sem, target):
        pl.semaphore_signal(
            sem, inc=1, device_id={"freq": target}, device_id_type=pl.DeviceIdType.MESH
        )

    def tell_line(sem):
        @pl.when(col > 0)
        def _():
            tell(sem, seat(col - 1, row, core))

        @pl.when(col < cols - 1)
        def _():
            tell(sem, seat(col + 1, row, core))

    beside = jnp.minimum(col, 1) + jnp.minimum(cols - 1 - col, 1)

    def at(k):
        return pl.ds(*steps[k])

    def lanes(core_at, k):
        return pl.ds(pl.multiple_of(core_at * half + steps[k][0], LANES), steps[k][1])

    def blocks_of(k):
        return pl.ds(packs[k][0] // LANES, packs[k][1] // LANES)

    def x_load(core_at, ref, sem, k):
        start, size = packs[k]
        for lane in range(start, start + size, LANES):
            origin = pl.ds(pl.multiple_of(core_at * half + lane, LANES), LANES)
            for fold in range(folds):
                pltpu.make_async_copy(
                    x_ref.at[:, fold, :, origin], ref.at[lane // LANES, fold], sem.at[k]
                ).start()

    def x_wait(ref, sem, k):
        whole = ref.at[blocks_of(k)]
        pltpu.make_async_copy(whole, whole, sem.at[k]).wait()

    def span_of(g):
        return pl.ds(*packs[g])

    def far_copy(g):
        return remote(
            p_send.at[:, :, :, :, span_of(g)],
            p_recv.at[:, :, :, :, span_of(g)],
            far_send,
            far_recv.at[g],
            mate,
        )

    def green_place(lane, side, part):
        return CORES * 2 * lane + (2 * side + part) * LANES

    def green_load(lane, side, part):
        core_at = core if side == 0 else 1 - core
        origin = pl.multiple_of(part * CORES * half + core_at * half + lane, LANES)
        return pltpu.make_async_copy(
            green_ref.at[pl.ds(origin, LANES), :],
            green_v.at[pl.ds(green_place(lane, side, part), LANES), :],
            green_sem,
        )

    fi_load = pltpu.make_async_copy(fi_hbm, fi_ref, load_sem.at[0])
    map_load = pltpu.make_async_copy(map_ref, map_v, load_sem.at[1])
    src_load = pltpu.make_async_copy(src_ref, src_v, load_sem.at[2])
    tell(barrier, mate)
    tell(barrier, across)
    x_load(1 - core, x_out, out_sem, order[0])
    fi_load.start()
    tell_line(barrier)
    for k, later in zip(order, order[1:]):
        x_load(1 - core, x_out, out_sem, later)
        x_load(core, x_near, near_sem, k)
    x_load(core, x_near, near_sem, order[-1])

    table_rows = 2 * freqs
    line = lax.broadcasted_iota(jnp.int32, (table_rows, samples), 0)
    column = lax.broadcasted_iota(jnp.int32, (table_rows, samples), 1)
    spread = lax.broadcasted_iota(jnp.int32, (samples, depth), 1) // SUBLANES == (
        lax.broadcasted_iota(jnp.int32, (samples, depth), 0)
    )
    fi_load.wait()
    bins = jnp.zeros((table_rows, samples), jnp.int32)
    for side in range(ROWS):
        for leg in range(LEGS):
            for k in range(CORES):
                to_row = 1 - row if side == 0 else row
                place = (side * LEGS + leg) * CORES + k
                bins = jnp.where(line // 2 == place, fi_ref[seat(leg_cols[leg], to_row, k)], bins)
    angles = lax.rem(bins * (me * samples + column), length).astype(f32) * f32(
        2.0 * math.pi / length
    )
    small = jnp.where(line % 2 == 0, jnp.cos(angles), -jnp.sin(angles)).astype(bf16)
    stretched = jnp.dot(small, jnp.where(spread, 1.0, 0.0).astype(bf16), preferred_element_type=f32)
    same_shot = lax.broadcasted_iota(jnp.int32, (SUBLANES, depth), 1) % SUBLANES == (
        lax.broadcasted_iota(jnp.int32, (SUBLANES, depth), 0)
    )
    for r in range(table_rows):
        spread_row = jnp.broadcast_to(stretched[r : r + 1, :], (SUBLANES, depth))
        table[r * SUBLANES : (r + 1) * SUBLANES, :] = jnp.where(same_shot, spread_row, 0.0).astype(
            bf16
        )

    def lanes_of(k):
        return range(packs[k][0], packs[k][0] + packs[k][1], LANES)

    def start_green(k):
        for lane in lanes_of(k):
            for side in range(CORES):
                for part in range(2):
                    green_load(lane, side, part).start()

    def transform(x_at, ref, g):
        start, size = packs[g]
        for fold in range(folds):
            seen = jnp.concatenate(
                [
                    x_at[start // LANES + n, fold].reshape(depth, LANES)
                    for n in range(size // LANES)
                ],
                axis=1,
            )
            total = jnp.dot(table[...], seen, preferred_element_type=f32)
            for side in range(ROWS):
                for leg in range(LEGS):
                    for line_at in range(2 * CORES):
                        first = ((side * LEGS + leg) * 2 * CORES + line_at) * SUBLANES
                        ref[side, leg, line_at * folds + fold, :, span_of(g)] = total[
                            first : first + SUBLANES
                        ].astype(ref.dtype)

    def hand_over(g):
        x_wait(x_out, out_sem, g)
        transform(x_out, p_send, g)

    def keep_near(g):
        x_wait(x_near, near_sem, g)
        transform(x_near, near, g)

    def y_copy(leg, k):
        return remote(
            y_send.at[leg, :, :, at(k)],
            y_recv.at[leg, :, :, at(k)],
            ys_sem,
            yr_sem.at[leg, k],
            across,
        )

    def pick(core_at):
        return pl.ds(core_at * groups, groups)

    def deliver(src_ref_at, kind, k, sem, arrived, to_col, to_row):
        for side in range(CORES):
            to_core = core if side == 0 else 1 - core
            remote(
                src_ref_at(to_core),
                fin.at[kind * CORES + side, :, :, at(k)],
                sem,
                arrived,
                seat(to_col, to_row, to_core),
            ).start()

    def last_copies(k):
        deliver(
            lambda c: y_send.at[LEGS - 1, pick(c), :, at(k)], 0, k, ys_sem, last_sem.at[k], col, 1 - row
        )

    def own_copy(k):
        return remote(
            own_send.at[:, :, at(k)], fin.at[3 * CORES, :, :, at(k)], os_sem, fin_sem.at[k], mate
        )

    def joint(side, leg, lane):
        return near[side, leg, :, :, lane] + p_recv[side, leg, :, :, lane].astype(f32)

    def send_partial(g):
        far_copy(g).wait_recv()
        for leg in range(LEGS):
            y_send[leg, :, :, span_of(g)] = joint(0, leg, span_of(g)).astype(bf16)

    def keep_partial(g):
        lane = span_of(g)
        for leg in range(LEGS):
            near[1, leg, :, :, lane] = joint(1, leg, lane)
        own_send[:, :, lane] = near[1, LEGS - 1, pick(1 - core), :, lane].astype(bf16)
        for m in members[g]:
            own_copy(m).start()

    def relay_copy(k):
        return remote(
            relay_send.at[:, :, at(k)],
            relay_recv.at[:, :, at(k)],
            rs_sem,
            rr_sem.at[k],
            seat(near_col, row, core),
        )

    def joined(leg, k):
        y_copy(leg, k).wait_recv()
        return near[1, leg, :, :, at(k)] + y_recv[leg, :, :, at(k)].astype(f32)

    def pass_on(k):
        relay_send[:, :, at(k)] = joined(0, k).astype(bf16)
        relay_copy(k).start()

    def cross(k):
        total = joined(1, k)
        relay_copy(k).wait_recv()
        cross_send[:, :, at(k)] = (total + relay_recv[:, :, at(k)].astype(f32)).astype(bf16)
        deliver(lambda c: cross_send.at[pick(c), :, at(k)], 2, k, cs_sem, fin_sem.at[k], cross_col, row)

    def close(k):
        close_send[:, :, at(k)] = joined(2, k).astype(bf16)
        deliver(lambda c: close_send.at[pick(c), :, at(k)], 1, k, ns_sem, fin_sem.at[k], near_col, row)

    def direct_copy(leg):
        return remote(
            d_send.at[leg], d_recv.at[leg], ds_sem, dr_sem, seat(leg_cols[leg], row, core)
        )

    def send_direct():
        far_copy(DIRECT).wait_recv()
        for leg in range(LEGS):
            for side in range(ROWS):
                total = joint(side, leg, span_of(DIRECT))
                places = pl.ds(side * CORES * groups, CORES * groups)
                if leg < LEGS - 1:
                    d_send[leg, places] = total.astype(bf16)
                else:
                    d_keep[places] = total
            if 0 < leg < LEGS - 1:
                direct_copy(leg).start()

    def join_direct():
        pltpu.make_async_copy(d_recv, d_recv, dr_sem).wait()
        total = d_keep[...]
        for leg in range(LEGS - 1):
            total = total + d_recv[leg].astype(f32)
        d_keep[...] = total
        d_sum[...] = total.astype(bf16)
        d_own[...] = d_keep[pl.ds((CORES + core) * groups, groups)]
        for slot, side, to_core, target in (
            (1, 0, core, across),
            (2, 0, 1 - core, seat(col, 1 - row, 1 - core)),
            (0, 1, 1 - core, mate),
        ):
            remote(
                d_sum.at[pl.ds((side * CORES + to_core) * groups, groups)],
                d_fin.at[slot],
                dp_sem,
                df_sem,
                target,
            ).start()

    tiles = map_v.shape[1]

    def make_mask():
        map_load.wait()
        pltpu.make_async_copy(green_v, green_v, green_sem).wait()
        in_tile = lax.broadcasted_iota(jnp.int32, (tiles, points), 1) // (
            points // tiles
        ) == lax.broadcasted_iota(jnp.int32, (tiles, points), 0)
        mask_v[...] = jnp.dot(
            map_v[...].astype(f32).astype(bf16),
            jnp.where(in_tile, 1.0, 0.0).astype(bf16),
            preferred_element_type=f32,
        )
        acc[...] = jnp.zeros_like(acc)

    deep = CORES * half // map_v.shape[0]

    def mask_chunk(k):
        for lane in lanes_of(k):
            for side in range(CORES):
                core_at = core if side == 0 else 1 - core
                for i in range(LANES // deep):
                    seen = mask_v[pl.ds((core_at * half + lane) // deep + i, 1), :]
                    seen = jnp.broadcast_to(seen, (deep, points)).astype(bf16)
                    for part in range(2):
                        place = green_place(lane, side, part) + i * deep
                        green_v[place : place + deep, :] = green_v[place : place + deep, :] * seen

    def use(start, size, totals):
        spectra = []
        for total in totals:
            spectrum = total.reshape(block, size) * f32(1.0 / math.sqrt(length))
            turned = jnp.concatenate((spectrum[block // 2 :], -spectrum[: block // 2]), axis=0)
            spectra += [spectrum, turned]
        parts = [
            spectrum[:, lane : lane + LANES] for lane in range(0, size, LANES) for spectrum in spectra
        ]
        whole = jnp.concatenate(parts, axis=1)
        high = whole.astype(bf16)
        low = (whole - high.astype(f32)).astype(bf16)
        both = jnp.dot(
            jnp.concatenate((high, low), axis=0),
            green_v[CORES * 2 * start : CORES * 2 * (start + size), :],
            preferred_element_type=f32,
        )
        acc[...] += both[:block] + both[block:]

    def consume(start, size, ks):
        lane = pl.ds(start, size)
        for k in ks:
            wait_fin(k)
        own = near[1, LEGS - 1, pick(core), :, lane]
        sums = []
        for side in range(CORES):
            total = own if side == 0 else fin[3 * CORES, :, :, lane].astype(f32)
            sums.append(
                total
                + fin[CORES + side, :, :, lane].astype(f32)
                + fin[2 * CORES + side, :, :, lane].astype(f32)
            )
        for k in ks:
            wait_last(k)
        use(start, size, [sums[side] + fin[side, :, :, lane].astype(f32) for side in range(CORES)])

    def consume_direct():
        pltpu.make_async_copy(d_fin, d_fin, df_sem).wait()
        use(
            *packs[DIRECT],
            [
                d_own[...] + d_fin[1].astype(f32),
                d_fin[0].astype(f32) + d_fin[2].astype(f32),
            ],
        )

    def wait_fin(k):
        five = fin.at[pl.ds(CORES, 2 * CORES + 1), :, :, at(k)]
        pltpu.make_async_copy(five, five, fin_sem.at[k]).wait()

    def wait_last(k):
        two = fin.at[pl.ds(0, CORES), :, :, at(k)]
        pltpu.make_async_copy(two, two, last_sem.at[k]).wait()

    wire = 0.7 / (2 * LANES)
    hop = 2.6
    clock = 0.0
    arrival = {}

    def expect(leg, k):
        nonlocal clock
        clock += steps[k][1] * wire
        arrival[leg, k] = clock

    def start_y(leg, ks):
        for k in ks:
            expect(leg, k)
            if leg < LEGS - 1:
                y_copy(leg, k).start()
            else:
                last_copies(k)

    def flat_of(groups_at):
        return [k for g in groups_at for k in members[g]]

    def combine(g):
        if g == DIRECT:
            send_direct()
            return
        send_partial(g)
        start_y(0, members[g])
        if g == folded[0]:
            start_y(1, members[g])
            clock_at_least(0.85)

    def clock_at_least(value):
        nonlocal clock
        clock = max(clock, value)

    def advance(token):
        kind, place = token[:2]
        g = order[place] if place < len(order) else None
        if kind == "M":
            hand_over(g)
            if place == 0:
                pl.semaphore_wait(barrier, 2 + beside)
                tell_line(line_sem.at[0])
            far_copy(g).start()
        elif kind == "N":
            keep_near(g)
        elif kind == "P":
            ahead = order[token[2]]
            x_wait(x_near, near_sem, g)
            x_wait(x_out, out_sem, ahead)
            transform(x_out, p_send, ahead)
            transform(x_near, near, g)
            far_copy(ahead).start()
        elif kind == "C":
            combine(g)
        elif kind == "K":
            keep_partial(folded[place])
        elif kind == "A":
            pl.semaphore_wait(line_sem.at[0], beside)
            tell_line(line_sem.at[1])
        else:
            pl.semaphore_wait(line_sem.at[1], beside)
            tell(pair_sem, mate)
            direct_copy(0).start()

    for step in PLAN:
        advance((step[0],) + tuple(int(digit) for digit in step[1:]))
    kept = sum(step[0] == "K" for step in PLAN)
    map_load.start()
    src_load.start()
    for g in range(len(packs)):
        start_green(g)
    turns = [(1, k) for k in flat_of(folded[1:])]
    others = [(2, k) for k in flat_of(folded)]
    if MIXED:
        led = turns[LEAD:]
        mixed = [t for pair in zip(others, led) for t in pair]
        turns = turns[:LEAD] + mixed + others[len(led) :]
    else:
        turns += others
    for leg, k in turns:
        start_y(leg, [k])
    tail = flat_of(folded[-1:])
    pl.semaphore_wait(pair_sem, 1)
    tell(row_sem, across)
    start_y(LEGS - 1, flat_of(folded[:-1]))

    def send_last():
        join_direct()
        for k in tail:
            last_copies(k)

    for k in tail:
        expect(LEGS - 1, k)
    events = [(6.2, 7, send_last), (MASK, 5, make_mask)]
    for place, g in enumerate(folded[kept:]):
        events.append((max(arrival[0, members[g][0]] - 0.6, 0.4), 8, lambda g=g: keep_partial(g)))
    mid = 0.0
    for g in folded:
        done = 0.0
        for k in members[g]:
            span = steps[k][1] * wire
            events.append((arrival[0, k], 0, lambda k=k: pass_on(k)))
            merged = max(arrival[1, k], arrival[0, k] + span + hop)
            events.append((merged, 1, lambda k=k: cross(k)))
            mid = max(mid, merged) + 2 * span
            events.append((arrival[2, k], 2, lambda k=k: close(k)))
            done = max(mid + hop + 0.5, arrival[2, k] + span + hop, arrival[LEGS - 1, k], done)
            if g in folded[len(folded) - SPLIT :]:
                events.append((done, 4, lambda k=k: consume(*steps[k], [k])))
        if g not in folded[len(folded) - SPLIT :]:
            events.append((done, 4, lambda g=g: consume(*packs[g], members[g])))
    events.append((done + LATE, 9, consume_direct))
    for g in range(len(packs)):
        events.append((MASK + 0.4 + 0.6 * g, 6, lambda g=g: mask_chunk(g)))
    for _, _, run in sorted(events, key=lambda e: e[:2]):
        run()

    src_load.wait()
    product = src_v[...].astype(f32) * acc[...]
    stacked = product[0:SUBLANES]
    for first in range(SUBLANES, block, SUBLANES):
        stacked = stacked + product[first : first + SUBLANES]
    flat[...] = jnp.sum(stacked, axis=0, keepdims=True)
    each = points // shards

    def window(d):
        first = jnp.minimum(d * each // LANES, points // LANES - 2)
        return pl.ds(pl.multiple_of(first * LANES, LANES), 2 * LANES)

    def i_copy(place):
        to = place + jnp.minimum(jnp.maximum(place + 1 - me, 0), 1)
        return remote(flat.at[:, window(to)], i_recv.at[me], is_sem, ir_sem, to)

    pl.semaphore_wait(row_sem, 1)
    for place in range(shards - 1):
        i_copy(place).start()
    i_recv[me] = flat[:, window(me)]
    others = i_recv.at[pl.ds(0, shards - 1)]
    rest = pl.ds(0, half - packs[DIRECT][1])
    for sent, sem in (
        (p_send, far_send),
        (y_send.at[:, :, :, rest], ys_sem),
        (relay_send.at[:, :, rest], rs_sem),
        (cross_send.at[:, :, rest], cs_sem),
        (close_send.at[:, :, rest], ns_sem),
        (own_send.at[:, :, rest], os_sem),
        (d_send, ds_sem),
        (d_fin, dp_sem),
    ):
        pltpu.make_async_copy(sent, sent, sem).wait()
    pltpu.make_async_copy(others, others, ir_sem).wait()
    total = i_recv[0]
    for slot in range(1, shards):
        total = total + i_recv[slot]
    first = jnp.minimum(me * each // LANES, points // LANES - 2) * LANES
    total = jnp.broadcast_to(total, (SUBLANES, 2 * LANES))
    shift = lax.rem(2 * LANES - (me * each - first), 2 * LANES)
    out_ref[...] = pltpu.roll(total, shift, 1)[0:1, :each]
    pltpu.make_async_copy(others, others, is_sem).wait()


def fused_body(traces, freq_index, block_map, green_rec, green_src):
    shards = lax.axis_size("freq")
    samples, receivers, shots = traces.shape
    points = green_rec.shape[3]
    freqs = freq_index.shape[0]
    half = receivers // CORES
    chunks = len(chunks_of(half))
    folds = shots // SUBLANES
    records = jnp.transpose(traces, (0, 2, 1)).reshape(samples, folds, SUBLANES, receivers)
    green = green_rec.reshape(2 * receivers, points)
    sources = green_src.reshape(2 * shots, points)
    block = 2 * shots
    groups = 2 * folds
    bf16, f32 = jnp.bfloat16, jnp.float32
    regular = pltpu.SemaphoreType.REGULAR
    outside = pl.BlockSpec(memory_space=pltpu.HBM)
    piece = (CORES * groups, SUBLANES, half)
    direct = (ROWS * CORES * groups, SUBLANES, groups_of(half)[DIRECT][1])
    image = pl.pallas_call(
        imaging_kernel,
        out_shape=jax.ShapeDtypeStruct((1, points // shards), f32),
        in_specs=[outside] * 5,
        out_specs=pl.BlockSpec(memory_space=pltpu.VMEM),
        scratch_shapes=[
            pltpu.SMEM(freq_index.shape, jnp.int32),
            pltpu.VMEM((half // LANES, folds, samples, SUBLANES, LANES), bf16),
            pltpu.VMEM((half // LANES, folds, samples, SUBLANES, LANES), bf16),
            pltpu.VMEM((2 * freqs * SUBLANES, samples * SUBLANES), bf16),
            pltpu.VMEM((ROWS, LEGS) + piece, bf16),
            pltpu.VMEM((ROWS, LEGS) + piece, bf16),
            pltpu.VMEM((ROWS, LEGS) + piece, f32),
            pltpu.VMEM((LEGS,) + piece, bf16),
            pltpu.VMEM((LEGS - 1,) + piece, bf16),
            pltpu.VMEM(piece, bf16),
            pltpu.VMEM(piece, bf16),
            pltpu.VMEM(piece, bf16),
            pltpu.VMEM(piece, bf16),
            pltpu.VMEM((groups, SUBLANES, half), bf16),
            pltpu.VMEM((3 * CORES + 1, groups, SUBLANES, half), bf16),
            pltpu.VMEM((LEGS - 1,) + direct, bf16),
            pltpu.VMEM(direct, f32),
            pltpu.VMEM((LEGS - 1,) + direct, bf16),
            pltpu.VMEM(direct, bf16),
            pltpu.VMEM((groups,) + direct[1:], f32),
            pltpu.VMEM((ROWS * CORES - 1, groups) + direct[1:], bf16),
            pltpu.VMEM((2 * receivers, points), bf16),
            pltpu.VMEM((block, points), bf16),
            pltpu.VMEM(block_map.shape, jnp.int32),
            pltpu.VMEM((block_map.shape[0], points), f32),
            pltpu.VMEM((block, points), f32),
            pltpu.VMEM((1, points), f32),
            pltpu.VMEM((shards, 1, 2 * LANES), f32),
            regular((PAIR,)),
            regular,
            regular,
        ],
        compiler_params=pltpu.CompilerParams(
            collective_id=0, has_side_effects=True, vmem_limit_bytes=48 * 1024 * 1024
        ),
    )(
        *(
            pltpu.with_memory_space_constraint(array, pltpu.HBM)
            for array in (records, freq_index, block_map, green, sources)
        )
    )
    return image.reshape(points // shards)


def moves_less(traces, freq_index, block_map, green_rec):
    shards = lax.axis_size("freq")
    samples, receivers, shots = traces.shape
    freqs = freq_index.shape[0]
    return (
        2 * freqs <= samples
        and freqs == shards
        and shards == 2 * PAIR * ROWS * CORES
        and shots % SUBLANES == 0
        and receivers % (CORES * LANES) == 0
        and receivers >= CORES * 5 * LANES
        and LANES % (receivers // block_map.shape[0]) == 0
        and green_rec.shape[3] % LANES == 0
        and green_rec.shape[3] >= 2 * LANES
        and green_rec.shape[3] // shards <= LANES
    )


def chosen_body(traces, freq_index, block_map, green_rec, green_src):
    fused = moves_less(traces, freq_index, block_map, green_rec)
    return (fused_body if fused else body)(traces, freq_index, block_map, green_rec, green_src)


def solution(mesh):
    in_specs = (
        P("freq", None, "groups"),
        P(),
        P(),
        P("freq", None, None, "groups"),
        P("freq", None, None, "groups"),
    )
    out_specs = P(("groups", "freq"))
    return jax.shard_map(chosen_body, mesh=mesh, in_specs=in_specs, out_specs=out_specs, check_vma=False)
```

```python
import functools
import math

import jax
import jax.numpy as jnp
from jax import lax
from jax.experimental import pallas as pl
from jax.experimental.pallas import tpu as pltpu
from jax.sharding import PartitionSpec as P


def dft_table(freq_index, length):
    sample_index = jnp.arange(length, dtype=jnp.int32)
    phases = freq_index[:, None] * sample_index[None, :] % length
    angles = phases.astype(jnp.float32) * jnp.float32(2.0 * math.pi / length)
    stacked = jnp.stack((jnp.cos(angles), -jnp.sin(angles)), axis=1)
    return stacked.reshape(freq_index.shape[0] * 2, length).astype(jnp.bfloat16)


def expand_map(block_map, receivers, points):
    row_span = receivers // block_map.shape[0]
    col_span = points // block_map.shape[1]
    return jnp.repeat(jnp.repeat(block_map, row_span, axis=0), col_span, axis=1).astype(
        jnp.bfloat16
    )


def transform(cos_table, records, length):
    spectrum = jnp.dot(cos_table, records.reshape(length, -1), preferred_element_type=jnp.float32)
    return (spectrum * (1.0 / math.sqrt(length))).astype(jnp.bfloat16)


def back_project(spectra, masked):
    swapped = jnp.stack((spectra[:, 1], -spectra[:, 0]), axis=1)
    blocks = jnp.stack((spectra, swapped), axis=1)
    return jnp.einsum("fcrx,focrs->fosx", masked, blocks, preferred_element_type=jnp.float32)


def body(traces, freq_index, block_map, green_rec, green_src):
    shards = lax.axis_size("freq")
    length = traces.shape[0] * shards
    receivers = traces.shape[1]
    shots = traces.shape[2]
    freqs = freq_index.shape[0]
    cos_table = dft_table(freq_index, length)
    masked = green_rec * expand_map(block_map, receivers, green_rec.shape[3])[None, None]
    regrouped = lax.all_to_all(traces, "freq", split_axis=2, concat_axis=0, tiled=True)
    spectrum = transform(cos_table, regrouped, length).reshape(freqs, 2, receivers, shots // shards)
    gathered = lax.all_to_all(spectrum, "freq", split_axis=0, concat_axis=3, tiled=True)
    back_field = back_project(gathered, masked)
    partial_image = jnp.sum(green_src.astype(jnp.float32) * back_field, axis=(0, 1, 2))
    return lax.psum_scatter(partial_image, "freq", scatter_dimension=0, tiled=True)


CORES = 2
ROWS = 2
PAIR = 2
LANES = 128
SUBLANES = 8
LEGS = 4
DIRECT = 1
WIDE = 2 * LANES
PIECE = LANES
AHEAD = 2
PLAN = ("M0", "P01", "P12", "P23", "C0", "C1", "A0", "P34", "C2", "N4", "C3", "B0", "C4", "K0", "K1")
MIXED = True
MASK = 3.6
LATE = -0.1
SPLIT = 1
LEAD = 0


def groups_of(half):
    sizes = [LANES, LANES]
    while sum(sizes) < half:
        sizes.append(min(WIDE, half - sum(sizes)))
    return tuple((sum(sizes[:k]), size) for k, size in enumerate(sizes))


def pieces_of(group):
    start, size = group
    return tuple((lane, min(PIECE, start + size - lane)) for lane in range(start, start + size, PIECE))


def chunks_of(half):
    return tuple(piece for group in groups_of(half) for piece in pieces_of(group))


def seat(col, row, core):
    return (col * ROWS + row) * CORES + core


def remote(src, dst, send_sem, recv_sem, target):
    return pltpu.make_async_remote_copy(
        src_ref=src,
        dst_ref=dst,
        send_sem=send_sem,
        recv_sem=recv_sem,
        device_id={"freq": target},
        device_id_type=pl.DeviceIdType.MESH,
    )


def imaging_kernel(*refs):
    half = refs[8].shape[0] * LANES
    chunks = len(chunks_of(half))
    packs = len(groups_of(half))
    dma = pltpu.SemaphoreType.DMA
    pl.run_scoped(
        functools.partial(imaging, *refs),
        dma((packs,)),
        dma((packs,)),
        dma((3,)),
        dma,
        dma,
        dma((packs,)),
        dma,
        dma((LEGS - 1, chunks)),
        dma,
        dma((chunks,)),
        dma,
        dma,
        dma,
        dma((chunks,)),
        dma((chunks,)),
        dma,
        dma,
        dma,
        dma,
        dma,
        dma,
    )


def imaging(
    x_ref,
    fi_hbm,
    map_ref,
    green_ref,
    src_ref,
    out_ref,
    fi_ref,
    x_out,
    x_near,
    table,
    p_send,
    p_recv,
    near,
    y_send,
    y_recv,
    relay_send,
    relay_recv,
    cross_send,
    close_send,
    own_send,
    fin,
    d_send,
    d_keep,
    d_recv,
    d_sum,
    d_own,
    d_fin,
    green_v,
    src_v,
    map_v,
    mask_v,
    acc,
    flat,
    i_recv,
    line_sem,
    pair_sem,
    row_sem,
    out_sem,
    near_sem,
    load_sem,
    green_sem,
    far_send,
    far_recv,
    ys_sem,
    yr_sem,
    rs_sem,
    rr_sem,
    cs_sem,
    ns_sem,
    os_sem,
    fin_sem,
    last_sem,
    ds_sem,
    dr_sem,
    dp_sem,
    df_sem,
    is_sem,
    ir_sem,
):
    shards = i_recv.shape[0]
    cols = shards // (ROWS * CORES)
    blocks, folds, samples = x_near.shape[:3]
    half = blocks * LANES
    length = samples * shards
    steps = chunks_of(half)
    chunks = len(steps)
    packs = groups_of(half)
    members = [[k for k in range(chunks) if p <= steps[k][0] < p + n] for p, n in packs]
    folded = [g for g in range(len(packs)) if g != DIRECT]
    order = folded[:AHEAD] + [DIRECT] + folded[AHEAD:]
    freqs = fi_ref.shape[0]
    points = acc.shape[1]
    block = acc.shape[0]
    groups = 2 * folds
    depth = samples * SUBLANES
    bf16, f32 = jnp.bfloat16, jnp.float32

    me = lax.axis_index("freq")
    core = lax.rem(me, CORES)
    row = lax.rem(me // CORES, ROWS)
    col = me // (CORES * ROWS)
    near_col = col + 1 - 2 * lax.rem(col, PAIR)
    cross_col = lax.rem(col + PAIR, cols)
    far_col = lax.rem(near_col + PAIR, cols)
    leg_cols = (far_col, cross_col, near_col, col)
    mate = seat(col, row, 1 - core)
    across = seat(col, 1 - row, core)

    barrier = pltpu.get_barrier_semaphore()

    def tell(sem, target):
        pl.semaphore_signal(
            sem, inc=1, device_id={"freq": target}, device_id_type=pl.DeviceIdType.MESH
        )

    def tell_line(sem):
        @pl.when(col > 0)
        def _():
            tell(sem, seat(col - 1, row, core))

        @pl.when(col < cols - 1)
        def _():
            tell(sem, seat(col + 1, row, core))

    beside = jnp.minimum(col, 1) + jnp.minimum(cols - 1 - col, 1)

    def at(k):
        return pl.ds(*steps[k])

    def lanes(core_at, k):
        return pl.ds(pl.multiple_of(core_at * half + steps[k][0], LANES), steps[k][1])

    def blocks_of(k):
        return pl.ds(packs[k][0] // LANES, packs[k][1] // LANES)

    def x_load(core_at, ref, sem, k):
        start, size = packs[k]
        for lane in range(start, start + size, LANES):
            origin = pl.ds(pl.multiple_of(core_at * half + lane, LANES), LANES)
            for fold in range(folds):
                pltpu.make_async_copy(
                    x_ref.at[:, fold, :, origin], ref.at[lane // LANES, fold], sem.at[k]
                ).start()

    def x_wait(ref, sem, k):
        whole = ref.at[blocks_of(k)]
        pltpu.make_async_copy(whole, whole, sem.at[k]).wait()

    def span_of(g):
        return pl.ds(*packs[g])

    def far_copy(g):
        return remote(
            p_send.at[:, :, :, :, span_of(g)],
            p_recv.at[:, :, :, :, span_of(g)],
            far_send,
            far_recv.at[g],
            mate,
        )

    def green_place(lane, side, part):
        return CORES * 2 * lane + (2 * side + part) * LANES

    def green_load(lane, side, part):
        core_at = core if side == 0 else 1 - core
        origin = pl.multiple_of(part * CORES * half + core_at * half + lane, LANES)
        return pltpu.make_async_copy(
            green_ref.at[pl.ds(origin, LANES), :],
            green_v.at[pl.ds(green_place(lane, side, part), LANES), :],
            green_sem,
        )

    fi_load = pltpu.make_async_copy(fi_hbm, fi_ref, load_sem.at[0])
    map_load = pltpu.make_async_copy(map_ref, map_v, load_sem.at[1])
    src_load = pltpu.make_async_copy(src_ref, src_v, load_sem.at[2])
    tell(barrier, mate)
    tell(barrier, across)
    x_load(1 - core, x_out, out_sem, order[0])
    fi_load.start()
    tell_line(barrier)
    for k, later in zip(order, order[1:]):
        x_load(1 - core, x_out, out_sem, later)
        x_load(core, x_near, near_sem, k)
    x_load(core, x_near, near_sem, order[-1])

    table_rows = 2 * freqs
    line = lax.broadcasted_iota(jnp.int32, (table_rows, samples), 0)
    column = lax.broadcasted_iota(jnp.int32, (table_rows, samples), 1)
    spread = lax.broadcasted_iota(jnp.int32, (samples, depth), 1) // SUBLANES == (
        lax.broadcasted_iota(jnp.int32, (samples, depth), 0)
    )
    fi_load.wait()
    bins = jnp.zeros((table_rows, samples), jnp.int32)
    for side in range(ROWS):
        for leg in range(LEGS):
            for k in range(CORES):
                to_row = 1 - row if side == 0 else row
                place = (side * LEGS + leg) * CORES + k
                bins = jnp.where(line // 2 == place, fi_ref[seat(leg_cols[leg], to_row, k)], bins)
    angles = lax.rem(bins * (me * samples + column), length).astype(f32) * f32(
        2.0 * math.pi / length
    )
    small = jnp.where(line % 2 == 0, jnp.cos(angles), -jnp.sin(angles)).astype(bf16)
    stretched = jnp.dot(small, jnp.where(spread, 1.0, 0.0).astype(bf16), preferred_element_type=f32)
    same_shot = lax.broadcasted_iota(jnp.int32, (SUBLANES, depth), 1) % SUBLANES == (
        lax.broadcasted_iota(jnp.int32, (SUBLANES, depth), 0)
    )
    for r in range(table_rows):
        spread_row = jnp.broadcast_to(stretched[r : r + 1, :], (SUBLANES, depth))
        table[r * SUBLANES : (r + 1) * SUBLANES, :] = jnp.where(same_shot, spread_row, 0.0).astype(
            bf16
        )

    def lanes_of(k):
        return range(packs[k][0], packs[k][0] + packs[k][1], LANES)

    def start_green(k):
        for lane in lanes_of(k):
            for side in range(CORES):
                for part in range(2):
                    green_load(lane, side, part).start()

    def transform(x_at, ref, g):
        start, size = packs[g]
        for fold in range(folds):
            seen = jnp.concatenate(
                [
                    x_at[start // LANES + n, fold].reshape(depth, LANES)
                    for n in range(size // LANES)
                ],
                axis=1,
            )
            total = jnp.dot(table[...], seen, preferred_element_type=f32)
            for side in range(ROWS):
                for leg in range(LEGS):
                    for line_at in range(2 * CORES):
                        first = ((side * LEGS + leg) * 2 * CORES + line_at) * SUBLANES
                        ref[side, leg, line_at * folds + fold, :, span_of(g)] = total[
                            first : first + SUBLANES
                        ].astype(ref.dtype)

    def hand_over(g):
        x_wait(x_out, out_sem, g)
        transform(x_out, p_send, g)

    def keep_near(g):
        x_wait(x_near, near_sem, g)
        transform(x_near, near, g)

    def y_copy(leg, k):
        return remote(
            y_send.at[leg, :, :, at(k)],
            y_recv.at[leg, :, :, at(k)],
            ys_sem,
            yr_sem.at[leg, k],
            across,
        )

    def pick(core_at):
        return pl.ds(core_at * groups, groups)

    def deliver(src_ref_at, kind, k, sem, arrived, to_col, to_row):
        for side in range(CORES):
            to_core = core if side == 0 else 1 - core
            remote(
                src_ref_at(to_core),
                fin.at[kind * CORES + side, :, :, at(k)],
                sem,
                arrived,
                seat(to_col, to_row, to_core),
            ).start()

    def last_copies(k):
        deliver(
            lambda c: y_send.at[LEGS - 1, pick(c), :, at(k)], 0, k, ys_sem, last_sem.at[k], col, 1 - row
        )

    def own_copy(k):
        return remote(
            own_send.at[:, :, at(k)], fin.at[3 * CORES, :, :, at(k)], os_sem, fin_sem.at[k], mate
        )

    def joint(side, leg, lane):
        return near[side, leg, :, :, lane] + p_recv[side, leg, :, :, lane].astype(f32)

    def send_partial(g):
        far_copy(g).wait_recv()
        for leg in range(LEGS):
            y_send[leg, :, :, span_of(g)] = joint(0, leg, span_of(g)).astype(bf16)

    def keep_partial(g):
        lane = span_of(g)
        for leg in range(LEGS):
            near[1, leg, :, :, lane] = joint(1, leg, lane)
        own_send[:, :, lane] = near[1, LEGS - 1, pick(1 - core), :, lane].astype(bf16)
        for m in members[g]:
            own_copy(m).start()

    def relay_copy(k):
        return remote(
            relay_send.at[:, :, at(k)],
            relay_recv.at[:, :, at(k)],
            rs_sem,
            rr_sem.at[k],
            seat(near_col, row, core),
        )

    def joined(leg, k):
        y_copy(leg, k).wait_recv()
        return near[1, leg, :, :, at(k)] + y_recv[leg, :, :, at(k)].astype(f32)

    def pass_on(k):
        relay_send[:, :, at(k)] = joined(0, k).astype(bf16)
        relay_copy(k).start()

    def cross(k):
        total = joined(1, k)
        relay_copy(k).wait_recv()
        cross_send[:, :, at(k)] = (total + relay_recv[:, :, at(k)].astype(f32)).astype(bf16)
        deliver(lambda c: cross_send.at[pick(c), :, at(k)], 2, k, cs_sem, fin_sem.at[k], cross_col, row)

    def close(k):
        close_send[:, :, at(k)] = joined(2, k).astype(bf16)
        deliver(lambda c: close_send.at[pick(c), :, at(k)], 1, k, ns_sem, fin_sem.at[k], near_col, row)

    def direct_copy(leg):
        return remote(
            d_send.at[leg], d_recv.at[leg], ds_sem, dr_sem, seat(leg_cols[leg], row, core)
        )

    def send_direct():
        far_copy(DIRECT).wait_recv()
        for leg in range(LEGS):
            for side in range(ROWS):
                total = joint(side, leg, span_of(DIRECT))
                places = pl.ds(side * CORES * groups, CORES * groups)
                if leg < LEGS - 1:
                    d_send[leg, places] = total.astype(bf16)
                else:
                    d_keep[places] = total
            if 0 < leg < LEGS - 1:
                direct_copy(leg).start()

    def join_direct():
        pltpu.make_async_copy(d_recv, d_recv, dr_sem).wait()
        total = d_keep[...]
        for leg in range(LEGS - 1):
            total = total + d_recv[leg].astype(f32)
        d_keep[...] = total
        d_sum[...] = total.astype(bf16)
        d_own[...] = d_keep[pl.ds((CORES + core) * groups, groups)]
        for slot, side, to_core, target in (
            (1, 0, core, across),
            (2, 0, 1 - core, seat(col, 1 - row, 1 - core)),
            (0, 1, 1 - core, mate),
        ):
            remote(
                d_sum.at[pl.ds((side * CORES + to_core) * groups, groups)],
                d_fin.at[slot],
                dp_sem,
                df_sem,
                target,
            ).start()

    tiles = map_v.shape[1]

    def make_mask():
        map_load.wait()
        pltpu.make_async_copy(green_v, green_v, green_sem).wait()
        in_tile = lax.broadcasted_iota(jnp.int32, (tiles, points), 1) // (
            points // tiles
        ) == lax.broadcasted_iota(jnp.int32, (tiles, points), 0)
        mask_v[...] = jnp.dot(
            map_v[...].astype(f32).astype(bf16),
            jnp.where(in_tile, 1.0, 0.0).astype(bf16),
            preferred_element_type=f32,
        )
        acc[...] = jnp.zeros_like(acc)

    deep = CORES * half // map_v.shape[0]

    def mask_chunk(k):
        for lane in lanes_of(k):
            for side in range(CORES):
                core_at = core if side == 0 else 1 - core
                for i in range(LANES // deep):
                    seen = mask_v[pl.ds((core_at * half + lane) // deep + i, 1), :]
                    seen = jnp.broadcast_to(seen, (deep, points)).astype(bf16)
                    for part in range(2):
                        place = green_place(lane, side, part) + i * deep
                        green_v[place : place + deep, :] = green_v[place : place + deep, :] * seen

    def use(start, size, totals):
        spectra = []
        for total in totals:
            spectrum = total.reshape(block, size) * f32(1.0 / math.sqrt(length))
            turned = jnp.concatenate((spectrum[block // 2 :], -spectrum[: block // 2]), axis=0)
            spectra += [spectrum, turned]
        parts = [
            spectrum[:, lane : lane + LANES] for lane in range(0, size, LANES) for spectrum in spectra
        ]
        whole = jnp.concatenate(parts, axis=1)
        high = whole.astype(bf16)
        low = (whole - high.astype(f32)).astype(bf16)
        both = jnp.dot(
            jnp.concatenate((high, low), axis=0),
            green_v[CORES * 2 * start : CORES * 2 * (start + size), :],
            preferred_element_type=f32,
        )
        acc[...] += both[:block] + both[block:]

    def consume(start, size, ks):
        lane = pl.ds(start, size)
        for k in ks:
            wait_fin(k)
        own = near[1, LEGS - 1, pick(core), :, lane]
        sums = []
        for side in range(CORES):
            total = own if side == 0 else fin[3 * CORES, :, :, lane].astype(f32)
            sums.append(
                total
                + fin[CORES + side, :, :, lane].astype(f32)
                + fin[2 * CORES + side, :, :, lane].astype(f32)
            )
        for k in ks:
            wait_last(k)
        use(start, size, [sums[side] + fin[side, :, :, lane].astype(f32) for side in range(CORES)])

    def consume_direct():
        pltpu.make_async_copy(d_fin, d_fin, df_sem).wait()
        use(
            *packs[DIRECT],
            [
                d_own[...] + d_fin[1].astype(f32),
                d_fin[0].astype(f32) + d_fin[2].astype(f32),
            ],
        )

    def wait_fin(k):
        five = fin.at[pl.ds(CORES, 2 * CORES + 1), :, :, at(k)]
        pltpu.make_async_copy(five, five, fin_sem.at[k]).wait()

    def wait_last(k):
        two = fin.at[pl.ds(0, CORES), :, :, at(k)]
        pltpu.make_async_copy(two, two, last_sem.at[k]).wait()

    wire = 0.7 / (2 * LANES)
    hop = 2.6
    clock = 0.0
    arrival = {}

    def expect(leg, k):
        nonlocal clock
        clock += steps[k][1] * wire
        arrival[leg, k] = clock

    def start_y(leg, ks):
        for k in ks:
            expect(leg, k)
            if leg < LEGS - 1:
                y_copy(leg, k).start()
            else:
                last_copies(k)

    def flat_of(groups_at):
        return [k for g in groups_at for k in members[g]]

    def combine(g):
        if g == DIRECT:
            send_direct()
            return
        send_partial(g)
        start_y(0, members[g])
        if g == folded[0]:
            start_y(1, members[g])
            clock_at_least(0.85)

    def clock_at_least(value):
        nonlocal clock
        clock = max(clock, value)

    def advance(token):
        kind, place = token[:2]
        g = order[place] if place < len(order) else None
        if kind == "M":
            hand_over(g)
            if place == 0:
                pl.semaphore_wait(barrier, 2 + beside)
                tell_line(line_sem.at[0])
            far_copy(g).start()
        elif kind == "N":
            keep_near(g)
        elif kind == "P":
            ahead = order[token[2]]
            x_wait(x_near, near_sem, g)
            x_wait(x_out, out_sem, ahead)
            transform(x_out, p_send, ahead)
            transform(x_near, near, g)
            far_copy(ahead).start()
        elif kind == "C":
            combine(g)
        elif kind == "K":
            keep_partial(folded[place])
        elif kind == "A":
            pl.semaphore_wait(line_sem.at[0], beside)
            tell_line(line_sem.at[1])
        else:
            pl.semaphore_wait(line_sem.at[1], beside)
            tell(pair_sem, mate)
            direct_copy(0).start()

    for step in PLAN:
        advance((step[0],) + tuple(int(digit) for digit in step[1:]))
    kept = sum(step[0] == "K" for step in PLAN)
    map_load.start()
    src_load.start()
    turns = [(1, k) for k in flat_of(folded[1:])]
    others = [(2, k) for k in flat_of(folded)]
    if MIXED:
        led = turns[LEAD:]
        mixed = [t for pair in zip(others, led) for t in pair]
        turns = turns[:LEAD] + mixed + others[len(led) :]
    else:
        turns += others
    for leg, k in turns:
        start_y(leg, [k])
    tail = flat_of(folded[-1:])
    pl.semaphore_wait(pair_sem, 1)
    tell(row_sem, across)
    start_y(LEGS - 1, flat_of(folded[:-1]))

    def send_last():
        join_direct()
        for k in tail:
            last_copies(k)

    for k in tail:
        expect(LEGS - 1, k)
    events = [(6.2, 7, send_last), (MASK, 5, make_mask)]
    for g in range(len(packs)):
        events.append((0.3 + 0.3 * g, 3, lambda g=g: start_green(g)))
    for place, g in enumerate(folded[kept:]):
        events.append((max(arrival[0, members[g][0]] - 0.6, 0.4), 8, lambda g=g: keep_partial(g)))
    mid = 0.0
    for g in folded:
        done = 0.0
        for k in members[g]:
            span = steps[k][1] * wire
            events.append((arrival[0, k], 0, lambda k=k: pass_on(k)))
            merged = max(arrival[1, k], arrival[0, k] + span + hop)
            events.append((merged, 1, lambda k=k: cross(k)))
            mid = max(mid, merged) + 2 * span
            events.append((arrival[2, k], 2, lambda k=k: close(k)))
            done = max(mid + hop + 0.5, arrival[2, k] + span + hop, arrival[LEGS - 1, k], done)
            if g in folded[len(folded) - SPLIT :]:
                events.append((done, 4, lambda k=k: consume(*steps[k], [k])))
        if g not in folded[len(folded) - SPLIT :]:
            events.append((done, 4, lambda g=g: consume(*packs[g], members[g])))
    events.append((done + LATE, 9, consume_direct))
    for g in range(len(packs)):
        events.append((MASK + 0.4 + 0.6 * g, 6, lambda g=g: mask_chunk(g)))
    for _, _, run in sorted(events, key=lambda e: e[:2]):
        run()

    src_load.wait()
    product = src_v[...].astype(f32) * acc[...]
    stacked = product[0:SUBLANES]
    for first in range(SUBLANES, block, SUBLANES):
        stacked = stacked + product[first : first + SUBLANES]
    flat[...] = jnp.sum(stacked, axis=0, keepdims=True)
    each = points // shards

    def window(d):
        first = jnp.minimum(d * each // LANES, points // LANES - 2)
        return pl.ds(pl.multiple_of(first * LANES, LANES), 2 * LANES)

    def i_copy(place):
        to = place + jnp.minimum(jnp.maximum(place + 1 - me, 0), 1)
        return remote(flat.at[:, window(to)], i_recv.at[me], is_sem, ir_sem, to)

    pl.semaphore_wait(row_sem, 1)
    for place in range(shards - 1):
        i_copy(place).start()
    i_recv[me] = flat[:, window(me)]
    others = i_recv.at[pl.ds(0, shards - 1)]
    rest = pl.ds(0, half - packs[DIRECT][1])
    for sent, sem in (
        (p_send, far_send),
        (y_send.at[:, :, :, rest], ys_sem),
        (relay_send.at[:, :, rest], rs_sem),
        (cross_send.at[:, :, rest], cs_sem),
        (close_send.at[:, :, rest], ns_sem),
        (own_send.at[:, :, rest], os_sem),
        (d_send, ds_sem),
        (d_fin, dp_sem),
    ):
        pltpu.make_async_copy(sent, sent, sem).wait()
    pltpu.make_async_copy(others, others, ir_sem).wait()
    total = i_recv[0]
    for slot in range(1, shards):
        total = total + i_recv[slot]
    first = jnp.minimum(me * each // LANES, points // LANES - 2) * LANES
    total = jnp.broadcast_to(total, (SUBLANES, 2 * LANES))
    shift = lax.rem(2 * LANES - (me * each - first), 2 * LANES)
    out_ref[...] = pltpu.roll(total, shift, 1)[0:1, :each]
    pltpu.make_async_copy(others, others, is_sem).wait()


def fused_body(traces, freq_index, block_map, green_rec, green_src):
    shards = lax.axis_size("freq")
    samples, receivers, shots = traces.shape
    points = green_rec.shape[3]
    freqs = freq_index.shape[0]
    half = receivers // CORES
    chunks = len(chunks_of(half))
    folds = shots // SUBLANES
    records = jnp.transpose(traces, (0, 2, 1)).reshape(samples, folds, SUBLANES, receivers)
    green = green_rec.reshape(2 * receivers, points)
    sources = green_src.reshape(2 * shots, points)
    block = 2 * shots
    groups = 2 * folds
    bf16, f32 = jnp.bfloat16, jnp.float32
    regular = pltpu.SemaphoreType.REGULAR
    outside = pl.BlockSpec(memory_space=pltpu.HBM)
    piece = (CORES * groups, SUBLANES, half)
    direct = (ROWS * CORES * groups, SUBLANES, groups_of(half)[DIRECT][1])
    image = pl.pallas_call(
        imaging_kernel,
        out_shape=jax.ShapeDtypeStruct((1, points // shards), f32),
        in_specs=[outside] * 5,
        out_specs=pl.BlockSpec(memory_space=pltpu.VMEM),
        scratch_shapes=[
            pltpu.SMEM(freq_index.shape, jnp.int32),
            pltpu.VMEM((half // LANES, folds, samples, SUBLANES, LANES), bf16),
            pltpu.VMEM((half // LANES, folds, samples, SUBLANES, LANES), bf16),
            pltpu.VMEM((2 * freqs * SUBLANES, samples * SUBLANES), bf16),
            pltpu.VMEM((ROWS, LEGS) + piece, bf16),
            pltpu.VMEM((ROWS, LEGS) + piece, bf16),
            pltpu.VMEM((ROWS, LEGS) + piece, f32),
            pltpu.VMEM((LEGS,) + piece, bf16),
            pltpu.VMEM((LEGS - 1,) + piece, bf16),
            pltpu.VMEM(piece, bf16),
            pltpu.VMEM(piece, bf16),
            pltpu.VMEM(piece, bf16),
            pltpu.VMEM(piece, bf16),
            pltpu.VMEM((groups, SUBLANES, half), bf16),
            pltpu.VMEM((3 * CORES + 1, groups, SUBLANES, half), bf16),
            pltpu.VMEM((LEGS - 1,) + direct, bf16),
            pltpu.VMEM(direct, f32),
            pltpu.VMEM((LEGS - 1,) + direct, bf16),
            pltpu.VMEM(direct, bf16),
            pltpu.VMEM((groups,) + direct[1:], f32),
            pltpu.VMEM((ROWS * CORES - 1, groups) + direct[1:], bf16),
            pltpu.VMEM((2 * receivers, points), bf16),
            pltpu.VMEM((block, points), bf16),
            pltpu.VMEM(block_map.shape, jnp.int32),
            pltpu.VMEM((block_map.shape[0], points), f32),
            pltpu.VMEM((block, points), f32),
            pltpu.VMEM((1, points), f32),
            pltpu.VMEM((shards, 1, 2 * LANES), f32),
            regular((PAIR,)),
            regular,
            regular,
        ],
        compiler_params=pltpu.CompilerParams(
            collective_id=0, has_side_effects=True, vmem_limit_bytes=48 * 1024 * 1024
        ),
    )(
        *(
            pltpu.with_memory_space_constraint(array, pltpu.HBM)
            for array in (records, freq_index, block_map, green, sources)
        )
    )
    return image.reshape(points // shards)


def moves_less(traces, freq_index, block_map, green_rec):
    shards = lax.axis_size("freq")
    samples, receivers, shots = traces.shape
    freqs = freq_index.shape[0]
    return (
        2 * freqs <= samples
        and freqs == shards
        and shards == 2 * PAIR * ROWS * CORES
        and shots % SUBLANES == 0
        and receivers % (CORES * LANES) == 0
        and receivers >= CORES * 5 * LANES
        and LANES % (receivers // block_map.shape[0]) == 0
        and green_rec.shape[3] % LANES == 0
        and green_rec.shape[3] >= 2 * LANES
        and green_rec.shape[3] // shards <= LANES
    )


def chosen_body(traces, freq_index, block_map, green_rec, green_src):
    fused = moves_less(traces, freq_index, block_map, green_rec)
    return (fused_body if fused else body)(traces, freq_index, block_map, green_rec, green_src)


def solution(mesh):
    in_specs = (
        P("freq", None, "groups"),
        P(),
        P(),
        P("freq", None, None, "groups"),
        P("freq", None, None, "groups"),
    )
    out_specs = P(("groups", "freq"))
    return jax.shard_map(chosen_body, mesh=mesh, in_specs=in_specs, out_specs=out_specs, check_vma=False)
```
